256 devices in a mesh: tp: 32 (over z, y), kv: 8 (over x, core).
Axes of the slice: x: 4, y: 4, z: 8, core: 2. Of those that a mesh axis runs over, the one named last changes fastest.
Arguments:
- hidden_in: bfloat16 [2048, 4096], P(('kv', 'tp')), may hold values from -6 to 6
- gain_attn: float32 [4096], replicated, may hold values from 0.4 to 1.6
- w_qkv: bfloat16 [4096, 32, 384], P(None, 'tp'), may hold values from -0.09375 to 0.09375
- cache_kv: bfloat16 [2, 8192, 32, 256], P(None, 'kv', 'tp'), may hold values from -110 to 110
- cache_len: int32 [2], replicated, may hold values from 128 to 8192, as said below
- w_out: bfloat16 [4096, 4096], P('tp'), may hold values from -0.1875 to 0.1875
- gain_mlp: float32 [4096], replicated, may hold values from 0.1 to 1.9
- w_gate_up: bfloat16 [4096, 2, 11008], P('kv', None, 'tp'), may hold values from -0.09375 to 0.09375
- w_down: bfloat16 [11008, 4096], P('tp', 'kv'), may hold values from -0.0546875 to 0.0546875
Outputs:
- layer_out: bfloat16 [2048, 4096], P(('kv', 'tp'))
The draws below stay inside these ranges and needn't reach their ends.
Inputs may be any that keep to these rules, and one draw needn't show every extreme that they name: `cache_len`: every length is a multiple of 128; some sequence uses the whole cache.
All inputs are finite; a program needn't handle non-finite values.
Results may differ from the reference program's by a relative error of at most 0.019.
The reference program's roundings to bfloat16 on the way count: a program that leaves them out, or rounds other values in their place, can miss the bound.
Values may be sent and summed in bfloat16 or wider, within the bound.
No kernel may reach another device: no remote copies, remote signals or barrier semaphores. Data moves between devices by JAX's collectives and lax.ppermute only.
A program may use at most 64 MiB of HBM per device.

```python
import math
import jax
import jax.numpy as jnp
from jax import lax

D = 4096
HEADS = 32
HEAD_SIZE = 128
FF = 11008
SPAN = 1024
CACHE = 8192
BATCH = 2
TOKENS = 2048


def draw_cache_kv(key, part):
    shape = (BATCH, CACHE, HEADS, 2 * HEAD_SIZE)
    return jnp.clip(jax.random.normal(key, shape, jnp.float32), -6.0, 6.0).astype(jnp.bfloat16)


def draw_cache_len(key, part):
    blocks = CACHE // 128
    order = jax.random.permutation(key, blocks)
    picked = order[jnp.arange(BATCH) % blocks]
    full_seq = jax.random.randint(jax.random.fold_in(key, 7), (), 0, BATCH)
    picked = jnp.where(jnp.arange(BATCH) == full_seq, blocks - 1, picked)
    return ((picked + 1) * 128).astype(jnp.int32)


def block_scale(own_key, dims, shards, smallest, high):
    def one(axis_at, parts):
        draws = jax.random.uniform(jax.random.fold_in(jax.random.fold_in(own_key, 6), axis_at), (parts,), jnp.float32, smallest / len(shards), high / len(shards))
        return jnp.repeat(jnp.exp(draws), dims[axis_at] // parts).reshape((-1,) + (1,) * (len(dims) - axis_at - 1))

    gain = one(*shards[0])
    for cut in shards[1:]:
        gain = gain * one(*cut)
    return gain


def centred(key, shape, spread, reach, cuts=(), kind=jnp.bfloat16):
    drawn = jax.random.normal(key, shape, jnp.float32) * spread
    if len(cuts) > 0:
        drawn = block_scale(key, shape, cuts, -0.22, 0.18) * drawn
    return jnp.clip(drawn, min=-reach, max=reach).astype(kind)


def setup_inputs(seed: int = 0) -> dict:
    key_list = jax.random.split(jax.random.key(seed), 10)
    hidden_in = centred(key_list[0], (TOKENS, D), 1.0, 6.0, ((0, 256),))
    gain_attn = jnp.clip(jax.random.uniform(key_list[1], (D,), jnp.float32, 0.4, 1.6), 0.4, 1.6)
    w_qkv = centred(key_list[2], (D, HEADS, 3 * HEAD_SIZE), D ** -0.5, 0.09375, ((1, 32),))
    cache_kv = draw_cache_kv(jax.random.fold_in(key_list[9], 71), 0)
    cache_len = draw_cache_len(jax.random.fold_in(key_list[9], 71), 0)
    w_out = centred(key_list[5], (HEADS * HEAD_SIZE, D), (HEADS * HEAD_SIZE // 4) ** -0.5, 0.1875, ((0, 32),))
    gain_mlp = jnp.clip(1.0 + 0.18 * jax.random.normal(key_list[6], (D,), jnp.float32), 0.1, 1.9)
    w_gate_up = centred(key_list[7], (D, 2, FF), D ** -0.5, 0.09375, ((0, 8), (2, 32)))
    w_down = centred(key_list[8], (FF, D), FF ** -0.5, 0.0546875, ((0, 32), (1, 8)))
    return dict(hidden_in=hidden_in, gain_attn=gain_attn, w_qkv=w_qkv, cache_kv=cache_kv, cache_len=cache_len, w_out=w_out, gain_mlp=gain_mlp, w_gate_up=w_gate_up, w_down=w_down)


EPSILON = 1e-05
MASKED = -1e+30

def rms_scale(values_in, gain_vector):
    widened = values_in.astype(jnp.float32)
    mean_square = lax.optimization_barrier(jnp.mean(widened * widened, axis=-1, keepdims=True))
    return (widened * lax.rsqrt(mean_square + EPSILON) * gain_vector.astype(jnp.float32)).astype(jnp.bfloat16)

def reference(hidden_in, gain_attn, w_qkv, cache_kv, cache_len, w_out, gain_mlp, w_gate_up, w_down):
    normed = rms_scale(hidden_in, gain_attn)
    flat_qkv = w_qkv.reshape(D, HEADS * 3 * HEAD_SIZE)
    packed = jnp.dot(normed, flat_qkv, preferred_element_type=jnp.float32).astype(jnp.bfloat16)
    packed = packed.reshape(BATCH, SPAN, HEADS, 3 * HEAD_SIZE).transpose(2, 0, 1, 3)
    cache_heads = cache_kv.transpose(2, 0, 1, 3)
    positions = jnp.arange(CACHE, dtype=jnp.int32)
    valid_cache = positions[None, :] < cache_len.astype(jnp.int32)[:, None]
    usable = jnp.concatenate([valid_cache, jnp.ones((BATCH, SPAN), dtype=bool)], axis=1)

    def one_head(pair):
        head_packed, head_cache = pair
        query_rows = head_packed[:, :, :HEAD_SIZE].astype(jnp.float32)
        joined_key_rows = jnp.concatenate([head_cache[:, :, :HEAD_SIZE], head_packed[:, :, HEAD_SIZE:2 * HEAD_SIZE]], axis=1).astype(jnp.float32)
        joined_value_rows = jnp.concatenate([head_cache[:, :, HEAD_SIZE:], head_packed[:, :, 2 * HEAD_SIZE:]], axis=1).astype(jnp.float32)
        logit_scores = jnp.einsum('nmz,nvz->nmv', query_rows, joined_key_rows) / math.sqrt(HEAD_SIZE)
        logit_scores = jnp.where(usable[:, None, :], logit_scores, MASKED)
        row_peak = lax.optimization_barrier(jnp.max(logit_scores, axis=2, keepdims=True))
        raw_weights = jnp.where(usable[:, None, :], jnp.exp(logit_scores - row_peak), 0.0)
        mass = lax.optimization_barrier(jnp.sum(raw_weights, axis=2))
        rounded_values = lax.optimization_barrier(raw_weights.astype(jnp.bfloat16))
        summed_output = jnp.einsum('qnu,quf->qnf', rounded_values.astype(jnp.float32), joined_value_rows)
        return (summed_output / mass[:, :, None]).astype(jnp.bfloat16)
    heads_out = lax.map(one_head, (packed, cache_heads))
    attended = heads_out.transpose(1, 2, 0, 3).reshape(TOKENS, HEADS * HEAD_SIZE)
    residual = hidden_in.astype(jnp.float32) + jnp.dot(attended, w_out, preferred_element_type=jnp.float32)
    mlp_in = rms_scale(residual, gain_mlp)
    gate = jnp.dot(mlp_in, w_gate_up[:, 0, :], preferred_element_type=jnp.float32)
    upward = jnp.dot(mlp_in, w_gate_up[:, 1, :], preferred_element_type=jnp.float32)
    activated = (jax.nn.silu(gate) * upward).astype(jnp.bfloat16)
    down_sum = jnp.dot(activated, w_down, preferred_element_type=jnp.float32)
    return (residual + down_sum).astype(jnp.bfloat16)
```

```python
import functools
import math

import jax
import jax.numpy as jnp
from jax import lax
from jax.experimental import pallas as pl
from jax.experimental.pallas import tpu as pltpu
from jax.sharding import Mesh
from jax.sharding import PartitionSpec as P

TP = ("z", "y")
KV = ("x", "c")
KV_TP = ("x", "c", "z", "y")

EPSILON = 1e-05
MASKED = -1e30
F32 = jnp.float32
BF16 = jnp.bfloat16


def shifted(value, axis, step):
    count = lax.axis_size(axis)
    return lax.ppermute(value, axis, [(i, (i + step) % count) for i in range(count)])


def gathered_turned(value, axis):
    return [value] + [shifted(value, axis, s) for s in range(1, lax.axis_size(axis))]


def dot(a, b, ca, cb):
    return lax.dot_general(a, b, (((ca,), (cb,)), ((), ())), preferred_element_type=F32)


def whole(shape):
    return pl.BlockSpec(shape, lambda *_: (0,) * len(shape))


def qkv_kernel(x_ref, gain_ref, w_ref, q_ref, k_ref, v_ref, inv_ref, acc_ref):
    step = pl.program_id(0)
    width = w_ref.shape[0]

    @pl.when(step == 0)
    def _():
        x = x_ref[...].astype(F32)
        inv_ref[...] = lax.rsqrt(jnp.mean(x * x, axis=1, keepdims=True) + EPSILON)
        acc_ref[...] = jnp.zeros_like(acc_ref)

    cols = pl.ds(pl.multiple_of(step * width, width), width)
    normed = (x_ref[:, cols].astype(F32) * inv_ref[...] * gain_ref[...]).astype(BF16)
    acc_ref[...] += dot(normed, w_ref[...], 1, 0)

    @pl.when(step == pl.num_programs(0) - 1)
    def _():
        size = q_ref.shape[1]
        q_ref[...] = acc_ref[:, :size].astype(BF16)
        k_ref[...] = acc_ref[:, size : 2 * size].astype(BF16)
        v_ref[...] = acc_ref[:, 2 * size :].astype(BF16)


def qkv(rows, gain, weights):
    count, width = rows.shape
    size = weights.shape[1] // 3
    steps = 4
    return pl.pallas_call(
        qkv_kernel,
        grid=(steps,),
        in_specs=[
            whole((count, width)),
            pl.BlockSpec((1, width // steps), lambda i: (0, i)),
            pl.BlockSpec((width // steps, 3 * size), lambda i: (i, 0)),
        ],
        out_specs=[whole((count, size))] * 3,
        out_shape=[jax.ShapeDtypeStruct((count, size), BF16)] * 3,
        scratch_shapes=[pltpu.VMEM((count, 1), F32), pltpu.VMEM((count, 3 * size), F32)],
        name="qkv",
    )(rows, gain.reshape(1, width), weights)


def split3(value):
    first = value.astype(BF16).astype(F32)
    second = (value - first).astype(BF16).astype(F32)
    return first, second, value - first - second


def attend_kernel(slots, info_ref, *refs):
    count = len(slots)
    k_ref, v_ref, cache_ref = refs[count : count + 3]
    size = k_ref.shape[1]
    scale = 1.0 / math.sqrt(size)
    for q_ref, out_ref, slot in zip(refs[:count], refs[count + 3 :], slots):
        seq = info_ref[0, slot]
        limit = info_ref[1, slot]
        own = info_ref[2, slot] > 0
        q = q_ref[...]
        s1 = dot(cache_ref[seq, :, :size], q, 1, 1) * scale
        s2 = dot(k_ref[...], q, 1, 1) * scale
        usable = lax.broadcasted_iota(jnp.int32, s1.shape, 0) < limit
        s1 = jnp.where(usable, s1, MASKED)
        s2 = jnp.where(own, s2, MASKED)
        peak = jnp.maximum(jnp.max(s1, axis=0, keepdims=True), jnp.max(s2, axis=0, keepdims=True))
        p1 = jnp.where(usable, jnp.exp(s1 - peak), 0.0)
        p2 = jnp.where(own, jnp.exp(s2 - peak), 0.0)
        mass = jnp.sum(p1, axis=0, keepdims=True) + jnp.sum(p2, axis=0, keepdims=True)
        acc = dot(cache_ref[seq, :, size:], p1.astype(BF16), 0, 0)
        acc += dot(v_ref[...], p2.astype(BF16), 0, 0)
        out_ref[:size, :] = acc.astype(BF16)
        row = lax.broadcasted_iota(jnp.int32, (16, q.shape[0]), 0)
        stats = jnp.zeros((16, q.shape[0]), F32)
        for at, part in enumerate(split3(peak) + split3(mass)):
            stats = jnp.where(row == at, part, stats)
        out_ref[size:, :] = stats.astype(BF16)


def attend(slots, info, queries, k, v, cache):
    count, size = k.shape
    return pl.pallas_call(
        functools.partial(attend_kernel, slots),
        grid_spec=pltpu.PrefetchScalarGridSpec(
            num_scalar_prefetch=1,
            grid=(1,),
            in_specs=[whole(k.shape)] * (len(slots) + 2) + [whole(cache.shape)],
            out_specs=[whole((size + 16, count))] * len(slots),
        ),
        out_shape=[jax.ShapeDtypeStruct((size + 16, count), BF16)] * len(slots),
        name="attend",
    )(info, *queries, k, v, cache)


def combine_kernel(*refs):
    *parts, out_ref = refs
    size = parts[0].shape[0] - 16
    lanes, rows, _ = out_ref.shape
    stats = [ref[size:, :].astype(F32) for ref in parts]
    peaks = [s[0:1] + s[1:2] + s[2:3] for s in stats]
    best = peaks[0]
    for peak in peaks[1:]:
        best = jnp.maximum(best, peak)
    mass = jnp.zeros_like(best)
    acc = jnp.zeros((size, best.shape[1]), F32)
    for ref, s, peak in zip(parts, stats, peaks):
        scaling = jnp.exp(peak - best)
        mass += (s[3:4] + s[4:5] + s[5:6]) * scaling
        acc += ref[:size, :].astype(F32) * scaling
    attended = (acc / mass).T.reshape(rows // 8, lanes, 8, size)
    for s in range(lanes):
        out_ref[s] = attended[:, s].reshape(rows, size).astype(BF16)


def combine(parts, lanes):
    size = parts[0].shape[0] - 16
    shape = (lanes, parts[0].shape[1] // lanes, size)
    return pl.pallas_call(
        combine_kernel, out_shape=jax.ShapeDtypeStruct(shape, BF16), name="combine"
    )(*parts)


def project_kernel(*refs):
    *ins, out_ref = refs
    half = len(ins) // 2
    acc = dot(ins[0][...], ins[half][...], 1, 0)
    for a, w in zip(ins[1:half], ins[half + 1 :]):
        acc += dot(a[...], w[...], 1, 0)
    out_ref[...] = acc.astype(BF16)


def project(heads, weights):
    rows, size = heads[0].shape
    width = weights[0].shape[1]
    steps = 4
    tile = width // steps
    return pl.pallas_call(
        project_kernel,
        grid=(steps,),
        in_specs=[whole((rows, size))] * len(heads)
        + [pl.BlockSpec((size, tile), lambda i: (0, i))] * len(weights),
        out_specs=pl.BlockSpec((rows, tile), lambda i: (0, i)),
        out_shape=jax.ShapeDtypeStruct((rows, width), BF16),
        name="project",
    )(*heads, *weights)


def residual_kernel(terms_ref, hidden_ref, gain_ref, residual_ref, normed_ref):
    total = terms_ref[0].astype(F32)
    for s in range(1, terms_ref.shape[0]):
        total += terms_ref[s].astype(F32)
    total += hidden_ref[...].astype(F32)
    residual_ref[...] = total
    inv = lax.rsqrt(jnp.mean(total * total, axis=1, keepdims=True) + EPSILON)
    normed_ref[...] = (total * inv * gain_ref[...]).astype(BF16)


def add_and_norm(terms, hidden, gain):
    return pl.pallas_call(
        residual_kernel,
        out_shape=[
            jax.ShapeDtypeStruct(hidden.shape, F32),
            jax.ShapeDtypeStruct(hidden.shape, BF16),
        ],
        name="residual",
    )(terms, hidden, gain.reshape(1, -1))


def gate_up_kernel(x_ref, w_ref, out_ref, gate_ref, up_ref):
    step = pl.program_id(0)

    @pl.when(step == 0)
    def _():
        gate_ref[...] = jnp.zeros_like(gate_ref)
        up_ref[...] = jnp.zeros_like(up_ref)

    x = x_ref[...]
    gate_ref[...] += dot(x, w_ref[0], 1, 1)
    up_ref[...] += dot(x, w_ref[1], 1, 1)

    @pl.when(step == pl.num_programs(0) - 1)
    def _():
        gate = gate_ref[...]
        out_ref[...] = (gate / (1.0 + jnp.exp(-gate)) * up_ref[...]).astype(BF16)


def gate_and_up(rows, weights):
    steps, _, hidden, depth = weights.shape
    count = rows.shape[0]
    return pl.pallas_call(
        gate_up_kernel,
        grid=(steps,),
        in_specs=[
            pl.BlockSpec((count, depth), lambda i: (0, i)),
            pl.BlockSpec((None, 2, hidden, depth), lambda i: (i, 0, 0, 0)),
        ],
        out_specs=whole((count, hidden)),
        out_shape=jax.ShapeDtypeStruct((count, hidden), BF16),
        scratch_shapes=[pltpu.VMEM((count, hidden), F32)] * 2,
        name="gate_up",
    )(rows, weights)


def down_kernel(x_ref, w_ref, *out_refs):
    lanes = len(out_refs)
    total = dot(x_ref[...], w_ref[...], 1, 0)
    rows, width = total.shape
    total = total.reshape(rows // (8 * lanes), lanes, 8, width)
    for s, ref in enumerate(out_refs):
        ref[...] = total[:, s].reshape(rows // lanes, width).astype(BF16)


def down(rows, weights, lanes):
    steps, hidden, width = weights.shape
    count = rows.shape[0]
    return pl.pallas_call(
        down_kernel,
        grid=(steps,),
        in_specs=[
            whole((count, hidden)),
            pl.BlockSpec((None, hidden, width), lambda i: (i, 0, 0)),
        ],
        out_specs=[pl.BlockSpec((count // lanes, width), lambda i: (0, i))] * lanes,
        out_shape=[jax.ShapeDtypeStruct((count // lanes, steps * width), BF16)] * lanes,
        name="down",
    )(rows, weights)


def per_device(
    hidden_in, gain_attn, w_qkv, cache_kv, cache_len, w_out, gain_mlp, w_gate_up, w_down
):
    depth, heads, packed = w_qkv.shape
    seqs, spots = cache_kv.shape[:2]
    groups, lanes, peers = lax.axis_size("z"), lax.axis_size("y"), lax.axis_size(KV)
    own_rows = hidden_in.shape[0]
    kv_index = lax.axis_index(KV)

    def gather_y(value):
        return jnp.concatenate(gathered_turned(value, "y"), axis=0)

    def gather_z(value):
        return lax.all_gather(value, "z", axis=0, tiled=True)

    rows_y = gather_y(hidden_in)
    rows_y, w_gate_up, w_down, w_out = lax.optimization_barrier(
        (rows_y, w_gate_up, w_down, w_out)
    )
    rows = gather_z(rows_y)
    gate_up_all = lax.all_gather(w_gate_up.transpose(1, 2, 0), KV)
    down_all = lax.all_gather(w_down, KV)
    w_heads = [w_out] + [shifted(w_out, "y", -s) for s in range(1, lanes)]
    q, k, v = qkv(rows, gain_attn, w_qkv.reshape(depth, packed))

    per_seq = peers // seqs
    cache = cache_kv.reshape(seqs, spots, cache_kv.shape[3])
    seq_of = ((kv_index + peers - jnp.arange(peers, dtype=jnp.int32)) & (peers - 1)) // per_seq
    limits = jnp.where(seq_of == 0, cache_len[0], cache_len[1]) - kv_index * spots
    info = jnp.stack([seq_of, limits, (seq_of == kv_index // per_seq).astype(jnp.int32)])
    queries = gathered_turned(q, KV)
    parts = []
    for first in range(0, peers, 4):
        slots = tuple(range(first, first + 4))
        done = attend(slots, info, queries[first : first + 4], k, v, cache)
        parts += [shifted(part, KV, -s) if s else part for s, part in zip(slots, done)]
    attended = combine(parts, lanes)

    attended, gate_up_all = lax.optimization_barrier((attended, gate_up_all))
    heads_here = [shifted(attended[s], "y", -s) if s else attended[s] for s in range(lanes)]
    terms = project(heads_here, w_heads)
    terms = lax.all_to_all(
        terms.reshape(groups, own_rows, depth), "z", split_axis=0, concat_axis=0, tiled=True
    )
    residual, normed = add_and_norm(terms, hidden_in, gain_mlp)

    normed, down_all = lax.optimization_barrier((normed, down_all))
    activated = gate_and_up(gather_z(gather_y(normed)), gate_up_all)
    pieces = down(activated, down_all, lanes)
    pieces = [shifted(piece, "y", -s) if s else piece for s, piece in enumerate(pieces)]
    summed = sum(piece.astype(F32) for piece in pieces).astype(BF16)
    arrived = lax.all_to_all(
        summed.reshape(groups, own_rows, depth), "z", split_axis=0, concat_axis=0, tiled=True
    )
    return (residual + arrived.astype(F32).sum(axis=0)).astype(BF16)


def solution(mesh):
    split = Mesh(mesh.devices.reshape(8, 4, 4, 2), ("z", "y", "x", "c"))
    in_specs = (
        P(KV_TP, None),
        P(),
        P(None, TP, None),
        P(None, KV, TP, None),
        P(),
        P(TP, None),
        P(),
        P(KV, None, TP),
        P(TP, KV),
    )
    return jax.shard_map(
        per_device, mesh=split, in_specs=in_specs, out_specs=P(KV_TP, None), check_vma=False
    )
```

```python
import functools
import math

import jax
import jax.numpy as jnp
from jax import lax
from jax.experimental import pallas as pl
from jax.experimental.pallas import tpu as pltpu
from jax.sharding import Mesh
from jax.sharding import PartitionSpec as P


TP = ("z", "y")
KV = ("x", "c")
KV_TP = ("x", "c", "z", "y")

EPSILON = 1e-05
MASKED = -1e30
LOG2E = 1.4426950408889634
F32 = jnp.float32
BF16 = jnp.bfloat16


def shifted(value, axis, step):
    count = lax.axis_size(axis)
    return lax.ppermute(value, axis, [(i, (i + step) % count) for i in range(count)])


def gathered_turned(value, axis):
    return [value] + [shifted(value, axis, s) for s in range(1, lax.axis_size(axis))]


def dot(a, b, ca, cb):
    return lax.dot_general(a, b, (((ca,), (cb,)), ((), ())), preferred_element_type=F32)


def whole(shape):
    return pl.BlockSpec(shape, lambda *_: (0,) * len(shape))


def fetch(sources, buffer, sems):
    for j, source in enumerate(sources):
        pltpu.make_async_copy(source, buffer.at[j], sems.at[j]).start()


def arrived(buffer, sems, j):
    pltpu.make_async_copy(buffer.at[j], buffer.at[j], sems.at[j]).wait()


ANYWHERE = pl.BlockSpec(memory_space=pl.ANY)


def project_rows(x_refs, gain_ref, w_ref, w_buf, sems):
    steps, width, packed = w_buf.shape
    fetch([w_ref.at[pl.ds(j * width, width)] for j in range(steps)], w_buf, sems)
    scales = []
    for ref in x_refs:
        x = ref[...].astype(F32)
        scales.append(lax.rsqrt(jnp.mean(x * x, axis=1, keepdims=True) + EPSILON))

    def body(j, acc):
        cols = pl.ds(pl.multiple_of(j * width, width), width)
        gain = gain_ref[:, cols]
        normed = jnp.concatenate(
            [(ref[:, cols].astype(F32) * inv * gain) for ref, inv in zip(x_refs, scales)], axis=0
        ).astype(BF16)
        arrived(w_buf, sems, j)
        return acc + dot(normed, w_buf[j], 1, 0)

    zero = jnp.zeros((rows_of(x_refs), packed), F32)
    return lax.fori_loop(0, steps, body, zero)


def qkv_first_kernel(gain_ref, w_ref, *refs):
    *x_refs, out_ref, w_buf, sems = refs
    out_ref[...] = project_rows(x_refs, gain_ref, w_ref, w_buf, sems).astype(BF16)


def qkv_last_kernel(gain_ref, w_ref, first_ref, *refs):
    *x_refs, q_ref, k_ref, v_ref, w_buf, sems = refs
    acc = project_rows(x_refs, gain_ref, w_ref, w_buf, sems).astype(BF16)
    size = q_ref.shape[1]
    done = first_ref.shape[0]
    for at, ref in enumerate((q_ref, k_ref, v_ref)):
        ref[:done] = first_ref[:, at * size : (at + 1) * size]
        ref[done:] = acc[:, at * size : (at + 1) * size]


def rows_of(blocks):
    return sum(block.shape[0] for block in blocks)


def cost(rows, weight):
    return pl.CostEstimate(
        flops=2 * rows * weight, transcendentals=0, bytes_accessed=2 * weight
    )


def qkv_first(blocks, gain, weights):
    depth, packed = weights.shape
    count = rows_of(blocks)
    return pl.pallas_call(
        qkv_first_kernel,
        grid=(1,),
        in_specs=[whole((1, depth)), ANYWHERE] + [whole(b.shape) for b in blocks],
        out_specs=whole((count, packed)),
        out_shape=jax.ShapeDtypeStruct((count, packed), BF16),
        scratch_shapes=[
            pltpu.VMEM((4, depth // 4, packed), BF16),
            pltpu.SemaphoreType.DMA((4,)),
        ],
        cost_estimate=cost(count, depth * packed),
        name="qkv_first",
    )(gain.reshape(1, depth), weights, *blocks)


def qkv_last(first, blocks, gain, weights):
    depth, packed = weights.shape
    count = rows_of(blocks) + first.shape[0]
    shape = (count, packed // 3)
    return pl.pallas_call(
        qkv_last_kernel,
        grid=(1,),
        in_specs=[whole((1, depth)), ANYWHERE, whole(first.shape)]
        + [whole(b.shape) for b in blocks],
        out_specs=[whole(shape)] * 3,
        out_shape=[jax.ShapeDtypeStruct(shape, BF16)] * 3,
        scratch_shapes=[
            pltpu.VMEM((4, depth // 4, packed), BF16),
            pltpu.SemaphoreType.DMA((4,)),
        ],
        cost_estimate=cost(count, depth * packed),
        name="qkv_last",
    )(gain.reshape(1, depth), weights, first, *blocks)


def split3(value):
    first = value.astype(BF16).astype(F32)
    second = (value - first).astype(BF16).astype(F32)
    return first, second, value - first - second


def stats_of(peak, mass):
    row = lax.broadcasted_iota(jnp.int32, (16, peak.shape[1]), 0)
    stats = jnp.zeros((16, peak.shape[1]), F32)
    for at, part in enumerate(split3(peak) + split3(mass)):
        stats = jnp.where(row == at, part, stats)
    return stats.astype(BF16)


def attend_kernel(slots, info_ref, *refs):
    count = len(slots)
    k_ref, v_ref, cache_ref = refs[count : count + 3]
    size = k_ref.shape[1]
    scale = LOG2E / math.sqrt(size)
    for q_ref, out_ref, slot in zip(refs[:count], refs[count + 3 :], slots):
        seq = info_ref[0, slot]
        limit = info_ref[1, slot]
        own = info_ref[2, slot] > 0
        for at in range(0, q_ref.shape[0], 256):
            q = q_ref[at : at + 256]
            s1 = dot(cache_ref[seq, :, :size], q, 1, 1) * scale
            s2 = dot(k_ref[...], q, 1, 1) * scale
            usable = lax.broadcasted_iota(jnp.int32, s1.shape, 0) < limit
            s1 = jnp.where(usable, s1, MASKED)
            s2 = jnp.where(own, s2, MASKED)
            top = jnp.maximum(jnp.max(s1, axis=0, keepdims=True), jnp.max(s2, axis=0, keepdims=True))
            peak = jnp.maximum(top, 0.1 * MASKED)
            p1 = jnp.exp2(s1 - peak)
            p2 = jnp.exp2(s2 - peak)
            mass = jnp.sum(p1, axis=0, keepdims=True) + jnp.sum(p2, axis=0, keepdims=True)
            acc = dot(cache_ref[seq, :, size:], p1.astype(BF16), 0, 0)
            acc += dot(v_ref[...], p2.astype(BF16), 0, 0)
            out_ref[:size, at : at + 256] = acc.astype(BF16)
            out_ref[size:, at : at + 256] = stats_of(peak, mass)


def attend(slots, info, queries, k, v, cache):
    count, size = k.shape
    shapes = [(size + 16, q.shape[0]) for q in queries]
    return pl.pallas_call(
        functools.partial(attend_kernel, slots),
        grid_spec=pltpu.PrefetchScalarGridSpec(
            num_scalar_prefetch=1,
            grid=(1,),
            in_specs=[whole(q.shape) for q in queries]
            + [whole(k.shape), whole(v.shape), whole(cache.shape)],
            out_specs=[whole(shape) for shape in shapes],
        ),
        out_shape=[jax.ShapeDtypeStruct(shape, BF16) for shape in shapes],
        cost_estimate=cost(rows_of(queries), 2 * size * (cache.shape[1] + count)),
        name="attend",
    )(info, *queries, k, v, cache)


def merged(parts, size):
    stats = [part[size:].astype(F32) for part in parts]
    peaks = [s[0:1] + s[1:2] + s[2:3] for s in stats]
    best = functools.reduce(jnp.maximum, peaks)
    mass = jnp.zeros_like(best)
    acc = jnp.zeros((size, best.shape[1]), F32)
    for part, s, peak in zip(parts, stats, peaks):
        scaling = jnp.exp2(peak - best)
        mass += (s[3:4] + s[4:5] + s[5:6]) * scaling
        acc += part[:size].astype(F32) * scaling
    return best, mass, acc


def merge_kernel(*refs):
    *parts, mine_ref, other_ref = refs
    size = mine_ref.shape[0] - 16
    half = mine_ref.shape[1]
    for ref, at in ((mine_ref, 0), (other_ref, half)):
        best, mass, acc = merged([part[:, at : at + half] for part in parts], size)
        ref[:size] = acc.astype(BF16)
        ref[size:] = stats_of(best, mass)


def merge(parts):
    height, width = parts[0].shape
    return pl.pallas_call(
        merge_kernel,
        out_shape=[jax.ShapeDtypeStruct((height, width // 2), BF16)] * 2,
        name="merge",
    )(*parts)


def combine_kernel(mine_ref, other_ref, out_ref):
    size = mine_ref.shape[0] - 16
    lanes, rows, _ = out_ref.shape
    _, mass, acc = merged([mine_ref[...], other_ref[...]], size)
    attended = (acc / mass).T.reshape(rows // 8, lanes, 8, size)
    for s in range(lanes):
        out_ref[s] = attended[:, s].reshape(rows, size).astype(BF16)


def combine(mine, other, lanes):
    height, width = mine.shape
    shape = (lanes, width // lanes, height - 16)
    return pl.pallas_call(
        combine_kernel, out_shape=jax.ShapeDtypeStruct(shape, BF16), name="combine"
    )(mine, other)


def project_kernel(spots_ref, *refs):
    *ins, out_ref = refs
    half = len(ins) // 2
    acc = dot(ins[0][...], ins[half][...], 1, 0)
    for a, w in zip(ins[1:half], ins[half + 1 :]):
        acc += dot(a[...], w[...], 1, 0)
    groups, rows, width = out_ref.shape
    acc = acc.reshape(groups, rows, width)
    for s in range(groups):
        out_ref[spots_ref[s]] = acc[s].astype(BF16)


def project(spots, heads, weights):
    rows, size = heads[0].shape
    width = weights[0].shape[1]
    groups = spots.shape[0]
    steps = 4
    tile = width // steps
    return pl.pallas_call(
        project_kernel,
        grid_spec=pltpu.PrefetchScalarGridSpec(
            num_scalar_prefetch=1,
            grid=(steps,),
            in_specs=[whole((rows, size))] * len(heads)
            + [pl.BlockSpec((size, tile), lambda i, _: (0, i))] * len(weights),
            out_specs=pl.BlockSpec((groups, rows // groups, tile), lambda i, _: (0, 0, i)),
        ),
        out_shape=jax.ShapeDtypeStruct((groups, rows // groups, width), BF16),
        name="project",
    )(spots, *heads, *weights)


def residual_kernel(terms_ref, hidden_ref, gain_ref, residual_ref, normed_ref):
    total = terms_ref[0].astype(F32)
    for s in range(1, terms_ref.shape[0]):
        total += terms_ref[s].astype(F32)
    total += hidden_ref[...].astype(F32)
    residual_ref[...] = total
    inv = lax.rsqrt(jnp.mean(total * total, axis=1, keepdims=True) + EPSILON)
    normed_ref[...] = (total * inv * gain_ref[...]).astype(BF16)


def add_and_norm(terms, hidden, gain):
    return pl.pallas_call(
        residual_kernel,
        out_shape=[
            jax.ShapeDtypeStruct(hidden.shape, F32),
            jax.ShapeDtypeStruct(hidden.shape, BF16),
        ],
        name="residual",
    )(terms, hidden, gain.reshape(1, -1))


def activated_rows(at_ref, x_refs, w_refs, w_buf, sems):
    fetch(w_refs, w_buf, sems)
    steps, _, hidden, depth = w_buf.shape

    def body(j, sums):
        cols = pl.ds(pl.multiple_of(at_ref[j] * depth, depth), depth)
        x = jnp.concatenate([ref[:, cols] for ref in x_refs], axis=0)
        arrived(w_buf, sems, j)
        gate, up = sums
        return gate + dot(x, w_buf[j, 0], 1, 1), up + dot(x, w_buf[j, 1], 1, 1)

    zero = jnp.zeros((rows_of(x_refs), hidden), F32)
    gate, up = lax.fori_loop(0, steps, body, (zero, zero))
    return gate / (1.0 + jnp.exp(-gate)) * up


def gate_up_first_kernel(at_ref, near_ref, far_ref, *refs):
    *x_refs, out_ref, w_buf, sems = refs
    w_refs = [ref.at[j] for ref in (near_ref, far_ref) for j in range(ref.shape[0])]
    out_ref[...] = activated_rows(at_ref, x_refs, w_refs, w_buf, sems).astype(BF16)


def gate_up_last_kernel(lanes, at_ref, first_ref, near_ref, far_ref, *refs):
    *ins, w_buf, sems = refs
    x_refs, out_refs = ins[:-lanes], ins[-lanes:]
    w_refs = [ref.at[j] for ref in (near_ref, far_ref) for j in range(ref.shape[0])]
    last = activated_rows(at_ref, x_refs, w_refs, w_buf, sems)
    both = jnp.concatenate([first_ref[...].astype(F32), last], axis=0)
    rows, width = both.shape
    both = both.reshape(rows // (8 * lanes), lanes, 8, width)
    for s, ref in enumerate(out_refs):
        ref[...] = both[:, s].reshape(rows // lanes, width).astype(BF16)


def gate_up(at, blocks, weights, lanes, first=None):
    count = rows_of(blocks)
    side, _, hidden, depth = weights[0].shape
    side *= len(weights)
    if first is None:
        kernel = gate_up_first_kernel
        more, outs, lead = [], [(count, hidden)], []
    else:
        kernel = functools.partial(gate_up_last_kernel, lanes)
        more, lead = [whole(first.shape)], [first]
        outs = [((count + first.shape[0]) // lanes, hidden)] * lanes
    return pl.pallas_call(
        kernel,
        grid_spec=pltpu.PrefetchScalarGridSpec(
            num_scalar_prefetch=1,
            grid=(1,),
            in_specs=more + [ANYWHERE] * len(weights) + [whole(b.shape) for b in blocks],
            out_specs=[whole(shape) for shape in outs],
            scratch_shapes=[
                pltpu.VMEM((side, 2, hidden, depth), BF16),
                pltpu.SemaphoreType.DMA((side,)),
            ],
        ),
        out_shape=[jax.ShapeDtypeStruct(shape, BF16) for shape in outs],
        cost_estimate=cost(count, 2 * hidden * depth * side),
        name="gate_up_first" if first is None else "gate_up_last",
    )(at, *lead, *weights, *blocks)


def down_kernel(lanes, at_ref, spots_ref, *refs):
    *ins, out_ref, w_buf, sems = refs
    x_refs, w_refs = ins[:lanes], ins[lanes:]
    fetch(w_refs, w_buf, sems)
    groups, rows, _ = out_ref.shape
    steps, width = w_buf.shape[0], w_buf.shape[3]

    @pl.loop(0, steps)
    def _(j):
        arrived(w_buf, sems, j)
        acc = dot(x_refs[0][...], w_buf[j, 0], 1, 0)
        for s in range(1, lanes):
            acc += dot(x_refs[s][...], w_buf[j, s], 1, 0)
        acc = acc.reshape(groups, rows, width)
        cols = pl.ds(pl.multiple_of(at_ref[j] * width, width), width)
        for s in range(groups):
            out_ref[spots_ref[s], :, cols] = acc[s].astype(BF16)


def down(at, spots, pieces, weights):
    lanes = len(pieces)
    groups = spots.shape[0]
    rows = pieces[0].shape[0]
    width = weights[0].shape[2]
    shape = (groups, rows // groups, width * len(weights))
    return pl.pallas_call(
        functools.partial(down_kernel, lanes),
        grid_spec=pltpu.PrefetchScalarGridSpec(
            num_scalar_prefetch=2,
            grid=(1,),
            in_specs=[whole(p.shape) for p in pieces] + [ANYWHERE] * len(weights),
            out_specs=whole(shape),
            scratch_shapes=[
                pltpu.VMEM((len(weights),) + weights[0].shape, BF16),
                pltpu.SemaphoreType.DMA((len(weights),)),
            ],
        ),
        out_shape=jax.ShapeDtypeStruct(shape, BF16),
        name="down",
    )(at, spots, *pieces, *weights)


def per_device(
    hidden_in, gain_attn, w_qkv, cache_kv, cache_len, w_out, gain_mlp, w_gate_up, w_down
):
    depth, _, packed = w_qkv.shape
    seqs, spots = cache_kv.shape[:2]
    groups, lanes, peers = lax.axis_size("z"), lax.axis_size("y"), lax.axis_size(KV)
    tied = lax.optimization_barrier
    w_qkv = w_qkv.reshape(depth, packed)
    x_at, c_at, z_at = lax.axis_index("x"), lax.axis_index("c"), lax.axis_index("z")
    kv_index = lax.axis_index(KV)
    step = jnp.arange(peers, dtype=jnp.int32)
    sides = lax.axis_size("x")
    weights_at = ((x_at + sides - (step & (sides - 1))) & (sides - 1)) * 2 + (
        (c_at + step // sides) & 1
    )
    sign = 1 - 2 * (step & 1)
    block_at = (z_at + groups + sign * ((step + 1) // 2)) & (groups - 1)

    def gather_y(value):
        return jnp.concatenate(gathered_turned(value, "y"), axis=0)

    def along_y(value):
        return [value] + [shifted(value, "y", -s) for s in range(1, lanes)]

    half = 2 * hidden_in.shape[0]
    r0 = gather_y(hidden_in)
    r0, w_gate_up, w_out, w_down = tied((r0, w_gate_up.transpose(1, 2, 0), w_out, w_down))
    f1, b1 = shifted(r0, "z", 1), shifted(r0, "z", -1)
    gates = gathered_turned(w_gate_up, "x")
    f2, b2 = shifted(f1, "z", 1), shifted(b1, "z", -1)
    w_heads = along_y(w_out)
    f3, b3 = shifted(f2, "z", 1), shifted(b2, "z", -1)
    downs = along_y(w_down)
    f4, b4 = shifted(f3[:half], "z", 1), shifted(b3[half:], "z", -1)
    first = qkv_first([r0, f1, b1, f2, b2], gain_attn, w_qkv)
    q, k, v = qkv_last(first, [f3, b3, f4, b4], gain_attn, w_qkv)

    cache = cache_kv.reshape(seqs, spots, cache_kv.shape[3])
    seq_of = ((x_at + sides - step[:sides]) & (sides - 1)) // (sides // seqs)
    limits = jnp.where(seq_of == 0, cache_len[0], cache_len[1]) - kv_index * spots
    info = jnp.stack([seq_of, limits, (seq_of == x_at // (sides // seqs)).astype(jnp.int32)])
    q = jnp.concatenate([q, shifted(q, "c", 1)], axis=0)
    queries = gathered_turned(q, "x")
    parts = list(attend((0,), info, queries[:1], k, v, cache))
    for slots in ((1, 3), (2,)):
        done = attend(slots, info, [queries[s] for s in slots], k, v, cache)
        parts += [shifted(part, "x", -s) for s, part in zip(slots, done)]
    downs = gathered_turned(jnp.stack(downs), "x")
    mine, other = merge(parts)
    other = shifted(other, "c", 1)
    attended = combine(mine, other, lanes)

    attended, gates = tied((attended, gates))
    gates = jnp.stack(gates)
    gates = [gates, shifted(gates, "c", 1)]
    heads_here = [shifted(attended[s], "y", -s) if s else attended[s] for s in range(lanes)]
    terms = project(block_at, heads_here, w_heads)
    terms = lax.all_to_all(terms, "z", split_axis=0, concat_axis=0, tiled=True)
    residual, normed = add_and_norm(terms, hidden_in, gain_mlp)
    normed, gates = tied((normed, gates))

    r0 = gather_y(normed)
    f1, b1 = shifted(r0, "z", 1), shifted(r0, "z", -1)
    f2, b2 = shifted(f1, "z", 1), shifted(b1, "z", -1)
    f3, b3 = shifted(f2, "z", 1), shifted(b2, "z", -1)
    f3, b3, downs = tied((f3, b3, downs))
    downs = downs + [shifted(d, "c", 1) for d in downs]
    f4, b4 = shifted(f3[:half], "z", 1), shifted(b3[half:], "z", -1)
    (first,) = gate_up(weights_at, [r0, f1, b1, f2, b2], gates, lanes)
    pieces = gate_up(weights_at, [f3, b3, f4, b4], gates, lanes, first)
    pieces = [shifted(piece, "y", -s) if s else piece for s, piece in enumerate(pieces)]
    summed = down(weights_at, block_at, pieces, downs)
    shares = lax.all_to_all(summed, "z", split_axis=0, concat_axis=0, tiled=True)
    return (residual + shares.astype(F32).sum(axis=0)).astype(BF16)


def solution(mesh):
    split = Mesh(mesh.devices.reshape(8, 4, 4, 2), ("z", "y", "x", "c"))
    in_specs = (
        P(KV_TP, None),
        P(),
        P(None, TP, None),
        P(None, KV, TP, None),
        P(),
        P(TP, None),
        P(),
        P(KV, None, TP),
        P(TP, KV),
    )
    return jax.shard_map(
        per_device, mesh=split, in_specs=in_specs, out_specs=P(KV_TP, None), check_vma=False
    )
```

```python
import functools
import math

import jax
import jax.numpy as jnp
from jax import lax
from jax.experimental import pallas as pl
from jax.experimental.pallas import tpu as pltpu
from jax.sharding import Mesh
from jax.sharding import PartitionSpec as P


TP = ("z", "y")
KV = ("x", "c")
KV_TP = ("x", "c", "z", "y")

EPSILON = 1e-05
MASKED = -1e30
LOG2E = 1.4426950408889634
F32 = jnp.float32
BF16 = jnp.bfloat16


def shifted(value, axis, step):
    count = lax.axis_size(axis)
    return lax.ppermute(value, axis, [(i, (i + step) % count) for i in range(count)])


def gathered_turned(value, axis):
    return [value] + [shifted(value, axis, s) for s in range(1, lax.axis_size(axis))]


def dot(a, b, ca, cb):
    return lax.dot_general(a, b, (((ca,), (cb,)), ((), ())), preferred_element_type=F32)


def whole(shape):
    return pl.BlockSpec(shape, lambda *_: (0,) * len(shape))


def fetch(sources, buffer, sems):
    for j, source in enumerate(sources):
        pltpu.make_async_copy(source, buffer.at[j], sems.at[j]).start()


def arrived(buffer, sems, j):
    pltpu.make_async_copy(buffer.at[j], buffer.at[j], sems.at[j]).wait()


ANYWHERE = pl.BlockSpec(memory_space=pl.ANY)


def project_rows(x_refs, gain_ref, w_ref, w_buf, sems):
    steps, width, packed = w_buf.shape
    fetch([w_ref.at[pl.ds(j * width, width)] for j in range(steps)], w_buf, sems)
    scales = []
    for ref in x_refs:
        x = ref[...].astype(F32)
        scales.append(lax.rsqrt(jnp.mean(x * x, axis=1, keepdims=True) + EPSILON))

    def body(j, acc):
        cols = pl.ds(pl.multiple_of(j * width, width), width)
        gain = gain_ref[:, cols]
        normed = jnp.concatenate(
            [(ref[:, cols].astype(F32) * inv * gain) for ref, inv in zip(x_refs, scales)], axis=0
        ).astype(BF16)
        arrived(w_buf, sems, j)
        return acc + dot(normed, w_buf[j], 1, 0)

    zero = jnp.zeros((rows_of(x_refs), packed), F32)
    return lax.fori_loop(0, steps, body, zero)


def qkv_first_kernel(gain_ref, w_ref, *refs):
    *x_refs, out_ref, w_buf, sems = refs
    out_ref[...] = project_rows(x_refs, gain_ref, w_ref, w_buf, sems).astype(BF16)


def qkv_last_kernel(gain_ref, w_ref, first_ref, *refs):
    *x_refs, q_ref, k_ref, v_ref, w_buf, sems = refs
    acc = project_rows(x_refs, gain_ref, w_ref, w_buf, sems).astype(BF16)
    size = q_ref.shape[1]
    done = first_ref.shape[0]
    for at, ref in enumerate((q_ref, k_ref, v_ref)):
        ref[:done] = first_ref[:, at * size : (at + 1) * size]
        ref[done:] = acc[:, at * size : (at + 1) * size]


def rows_of(blocks):
    return sum(block.shape[0] for block in blocks)


def cost(rows, weight):
    return pl.CostEstimate(
        flops=2 * rows * weight, transcendentals=0, bytes_accessed=2 * weight
    )


def qkv_first(blocks, gain, weights):
    depth, packed = weights.shape
    count = rows_of(blocks)
    return pl.pallas_call(
        qkv_first_kernel,
        grid=(1,),
        in_specs=[whole((1, depth)), ANYWHERE] + [whole(b.shape) for b in blocks],
        out_specs=whole((count, packed)),
        out_shape=jax.ShapeDtypeStruct((count, packed), BF16),
        scratch_shapes=[
            pltpu.VMEM((4, depth // 4, packed), BF16),
            pltpu.SemaphoreType.DMA((4,)),
        ],
        cost_estimate=cost(count, depth * packed),
        name="qkv_first",
    )(gain.reshape(1, depth), weights, *blocks)


def qkv_last(first, blocks, gain, weights):
    depth, packed = weights.shape
    count = rows_of(blocks) + first.shape[0]
    shape = (count, packed // 3)
    return pl.pallas_call(
        qkv_last_kernel,
        grid=(1,),
        in_specs=[whole((1, depth)), ANYWHERE, whole(first.shape)]
        + [whole(b.shape) for b in blocks],
        out_specs=[whole(shape)] * 3,
        out_shape=[jax.ShapeDtypeStruct(shape, BF16)] * 3,
        scratch_shapes=[
            pltpu.VMEM((4, depth // 4, packed), BF16),
            pltpu.SemaphoreType.DMA((4,)),
        ],
        cost_estimate=cost(count, depth * packed),
        name="qkv_last",
    )(gain.reshape(1, depth), weights, first, *blocks)


def split3(value):
    first = value.astype(BF16).astype(F32)
    second = (value - first).astype(BF16).astype(F32)
    return first, second, value - first - second


def stats_of(peak, mass):
    row = lax.broadcasted_iota(jnp.int32, (16, peak.shape[1]), 0)
    stats = jnp.zeros((16, peak.shape[1]), F32)
    for at, part in enumerate(split3(peak) + split3(mass)):
        stats = jnp.where(row == at, part, stats)
    return stats.astype(BF16)


def attend_kernel(slots, info_ref, *refs):
    count = len(slots)
    k_ref, v_ref, cache_ref = refs[count : count + 3]
    size = k_ref.shape[1]
    scale = LOG2E / math.sqrt(size)
    q_buf, out_buf = refs[-2:]
    for at, ref in enumerate(refs[:count]):
        q_buf[at] = ref[...]
    blocks = k_ref.shape[0]
    parts = q_buf.shape[1] // blocks

    @pl.loop(0, count * parts)
    def _(turn):
        which, part = turn // parts, turn % parts
        slot = slots[0] + which * (slots[-1] - slots[0])
        seq = info_ref[0, slot]
        limit = info_ref[1, slot]
        own = info_ref[2, slot] > 0
        at = pl.ds(pl.multiple_of(part * blocks, blocks), blocks)
        q = q_buf[which, at]
        s1 = dot(cache_ref[seq, :, :size], q, 1, 1) * scale
        s2 = dot(k_ref[...], q, 1, 1) * scale
        usable = lax.broadcasted_iota(jnp.int32, s1.shape, 0) < limit
        s1 = jnp.where(usable, s1, MASKED)
        s2 = jnp.where(own, s2, MASKED)
        top = jnp.maximum(jnp.max(s1, axis=0, keepdims=True), jnp.max(s2, axis=0, keepdims=True))
        peak = jnp.maximum(top, 0.1 * MASKED)
        p1 = jnp.exp2(s1 - peak)
        p2 = jnp.exp2(s2 - peak)
        mass = jnp.sum(p1, axis=0, keepdims=True) + jnp.sum(p2, axis=0, keepdims=True)
        acc = dot(cache_ref[seq, :, size:], p1.astype(BF16), 0, 0)
        acc += dot(v_ref[...], p2.astype(BF16), 0, 0)
        out_buf[which, :size, at] = acc.astype(BF16)
        out_buf[which, size:, at] = stats_of(peak, mass)

    for at, ref in enumerate(refs[count + 3 : -2]):
        ref[...] = out_buf[at]


def attend(slots, info, queries, k, v, cache):
    count, size = k.shape
    shapes = [(size + 16, q.shape[0]) for q in queries]
    return pl.pallas_call(
        functools.partial(attend_kernel, slots),
        grid_spec=pltpu.PrefetchScalarGridSpec(
            num_scalar_prefetch=1,
            grid=(1,),
            in_specs=[whole(q.shape) for q in queries]
            + [whole(k.shape), whole(v.shape), whole(cache.shape)],
            out_specs=[whole(shape) for shape in shapes],
            scratch_shapes=[
                pltpu.VMEM((len(slots),) + queries[0].shape, BF16),
                pltpu.VMEM((len(slots),) + shapes[0], BF16),
            ],
        ),
        out_shape=[jax.ShapeDtypeStruct(shape, BF16) for shape in shapes],
        cost_estimate=cost(rows_of(queries), 2 * size * (cache.shape[1] + count)),
        name="attend",
    )(info, *queries, k, v, cache)


def merged(parts, size):
    stats = [part[size:].astype(F32) for part in parts]
    peaks = [s[0:1] + s[1:2] + s[2:3] for s in stats]
    best = functools.reduce(jnp.maximum, peaks)
    mass = jnp.zeros_like(best)
    acc = jnp.zeros((size, best.shape[1]), F32)
    for part, s, peak in zip(parts, stats, peaks):
        scaling = jnp.exp2(peak - best)
        mass += (s[3:4] + s[4:5] + s[5:6]) * scaling
        acc += part[:size].astype(F32) * scaling
    return best, mass, acc


def merge_kernel(*refs):
    *parts, out_ref = refs
    cores, height, width = out_ref.shape
    size = height - 16
    for c in range(cores):
        cols = slice(c * width, (c + 1) * width)
        best, mass, acc = merged([part[:, cols] for part in parts], size)
        out_ref[c, :size] = acc.astype(BF16)
        out_ref[c, size:] = stats_of(best, mass)


def merge(parts, cores):
    height, width = parts[0].shape
    return pl.pallas_call(
        merge_kernel,
        out_shape=jax.ShapeDtypeStruct((cores, height, width // cores), BF16),
        name="merge",
    )(*parts)


def combine_kernel(turn_ref, parts_ref, out_ref):
    size = parts_ref.shape[1] - 16
    lanes, rows, _ = out_ref.shape
    _, mass, acc = merged([parts_ref[c] for c in range(parts_ref.shape[0])], size)
    attended = (acc / mass).T.reshape(rows // 8, lanes, 8, size)
    for s in range(lanes):
        out_ref[turn_ref[s]] = attended[:, s].reshape(rows, size).astype(BF16)


def combine(turn, parts):
    _, height, width = parts.shape
    lanes = turn.shape[0]
    shape = (lanes, width // lanes, height - 16)
    return pl.pallas_call(
        combine_kernel,
        grid_spec=pltpu.PrefetchScalarGridSpec(
            num_scalar_prefetch=1,
            grid=(1,),
            in_specs=[whole(parts.shape)],
            out_specs=whole(shape),
        ),
        out_shape=jax.ShapeDtypeStruct(shape, BF16),
        name="combine",
    )(turn, parts)


def project_kernel(spots_ref, ahead_ref, heads_ref, *refs):
    *w_refs, out_ref = refs
    heads = jnp.concatenate([heads_ref[ahead_ref[s]] for s in range(len(w_refs))], axis=1)
    acc = dot(heads, jnp.concatenate([w[...] for w in w_refs], axis=0), 1, 0)
    groups, rows, width = out_ref.shape
    acc = acc.reshape(groups, rows, width)
    for s in range(groups):
        out_ref[spots_ref[s]] = acc[s].astype(BF16)


def project(spots, ahead, heads, weights):
    _, rows, size = heads.shape
    width = weights[0].shape[1]
    groups = spots.shape[0]
    steps = 4
    tile = width // steps
    return pl.pallas_call(
        project_kernel,
        grid_spec=pltpu.PrefetchScalarGridSpec(
            num_scalar_prefetch=2,
            grid=(steps,),
            in_specs=[whole(heads.shape)]
            + [pl.BlockSpec((size, tile), lambda i, *_: (0, i))] * len(weights),
            out_specs=pl.BlockSpec((groups, rows // groups, tile), lambda i, *_: (0, 0, i)),
        ),
        out_shape=jax.ShapeDtypeStruct((groups, rows // groups, width), BF16),
        name="project",
    )(spots, ahead, heads, *weights)


def residual_kernel(terms_ref, hidden_ref, gain_ref, residual_ref, normed_ref):
    total = terms_ref[0].astype(F32)
    for s in range(1, terms_ref.shape[0]):
        total += terms_ref[s].astype(F32)
    total += hidden_ref[...].astype(F32)
    residual_ref[...] = total
    inv = lax.rsqrt(jnp.mean(total * total, axis=1, keepdims=True) + EPSILON)
    normed_ref[...] = (total * inv * gain_ref[...]).astype(BF16)


def add_and_norm(terms, hidden, gain):
    return pl.pallas_call(
        residual_kernel,
        out_shape=[
            jax.ShapeDtypeStruct(hidden.shape, F32),
            jax.ShapeDtypeStruct(hidden.shape, BF16),
        ],
        name="residual",
    )(terms, hidden, gain.reshape(1, -1))


def activated_rows(at_ref, x_refs, near_ref, far_ref, w_buf, sems):
    fetch([ref.at[j] for ref in (near_ref, far_ref) for j in range(ref.shape[0])], w_buf, sems)
    steps, _, hidden, depth = w_buf.shape

    def body(j, sums):
        cols = pl.ds(pl.multiple_of(at_ref[j] * depth, depth), depth)
        x = jnp.concatenate([ref[:, cols] for ref in x_refs], axis=0)
        arrived(w_buf, sems, j)
        gate, up = sums
        return gate + dot(w_buf[j, 0], x, 1, 1), up + dot(w_buf[j, 1], x, 1, 1)

    zero = jnp.zeros((hidden, rows_of(x_refs)), F32)
    gate, up = lax.fori_loop(0, steps, body, (zero, zero))
    return (gate / (1.0 + jnp.exp(-gate)) * up).T


def gate_up_first_kernel(at_ref, near_ref, far_ref, *refs):
    *x_refs, out_ref, w_buf, sems = refs
    out_ref[...] = activated_rows(at_ref, x_refs, near_ref, far_ref, w_buf, sems).astype(BF16)


def gate_up_last_kernel(at_ref, turn_ref, first_ref, near_ref, far_ref, *refs):
    *x_refs, out_ref, w_buf, sems = refs
    last = activated_rows(at_ref, x_refs, near_ref, far_ref, w_buf, sems)
    both = jnp.concatenate([first_ref[...].astype(F32), last], axis=0)
    rows, width = both.shape
    lanes = out_ref.shape[0]
    both = both.reshape(rows // (8 * lanes), lanes, 8, width)
    for s in range(lanes):
        out_ref[turn_ref[s]] = both[:, s].reshape(rows // lanes, width).astype(BF16)


def gate_up(at, blocks, weights, turn=None, first=None):
    count = rows_of(blocks)
    side, _, hidden, depth = weights[0].shape
    side *= len(weights)
    if first is None:
        kernel, lead, scalars = gate_up_first_kernel, [], [at]
        shape = (count, hidden)
    else:
        kernel, lead, scalars = gate_up_last_kernel, [first], [at, turn]
        lanes = turn.shape[0]
        shape = (lanes, (count + first.shape[0]) // lanes, hidden)
    return pl.pallas_call(
        kernel,
        grid_spec=pltpu.PrefetchScalarGridSpec(
            num_scalar_prefetch=len(scalars),
            grid=(1,),
            in_specs=[whole(value.shape) for value in lead]
            + [ANYWHERE] * len(weights)
            + [whole(b.shape) for b in blocks],
            out_specs=whole(shape),
            scratch_shapes=[
                pltpu.VMEM((side, 2, hidden, depth), BF16),
                pltpu.SemaphoreType.DMA((side,)),
            ],
        ),
        out_shape=jax.ShapeDtypeStruct(shape, BF16),
        cost_estimate=cost(count, 2 * hidden * depth * side),
        name="gate_up_first" if first is None else "gate_up_last",
    )(*scalars, *lead, *weights, *blocks)


def down_kernel(at_ref, spots_ref, ahead_ref, x_ref, *refs):
    *w_refs, out_ref, w_buf, sems = refs
    fetch(w_refs, w_buf, sems)
    groups, rows, _ = out_ref.shape
    steps, lanes, _, width = w_buf.shape

    @pl.loop(0, steps)
    def _(j):
        arrived(w_buf, sems, j)
        acc = dot(x_ref[ahead_ref[0]], w_buf[j, 0], 1, 0)
        for s in range(1, lanes):
            acc += dot(x_ref[ahead_ref[s]], w_buf[j, s], 1, 0)
        acc = acc.reshape(groups, rows, width)
        cols = pl.ds(pl.multiple_of(at_ref[j] * width, width), width)
        for s in range(groups):
            out_ref[spots_ref[s], :, cols] = acc[s].astype(BF16)


def down(at, spots, ahead, pieces, weights):
    groups = spots.shape[0]
    rows = pieces.shape[1]
    width = weights[0].shape[2]
    shape = (groups, rows // groups, width * len(weights))
    return pl.pallas_call(
        down_kernel,
        grid_spec=pltpu.PrefetchScalarGridSpec(
            num_scalar_prefetch=3,
            grid=(1,),
            in_specs=[whole(pieces.shape)] + [ANYWHERE] * len(weights),
            out_specs=whole(shape),
            scratch_shapes=[
                pltpu.VMEM((len(weights),) + weights[0].shape, BF16),
                pltpu.SemaphoreType.DMA((len(weights),)),
            ],
        ),
        out_shape=jax.ShapeDtypeStruct(shape, BF16),
        name="down",
    )(at, spots, ahead, pieces, *weights)


def per_device(
    hidden_in, gain_attn, w_qkv, cache_kv, cache_len, w_out, gain_mlp, w_gate_up, w_down
):
    depth, _, packed = w_qkv.shape
    seqs, spots = cache_kv.shape[:2]
    groups, lanes, peers = lax.axis_size("z"), lax.axis_size("y"), lax.axis_size(KV)
    tied = lax.optimization_barrier
    w_qkv = w_qkv.reshape(depth, packed)
    x_at, c_at, z_at = lax.axis_index("x"), lax.axis_index("c"), lax.axis_index("z")
    kv_index = lax.axis_index(KV)
    step = jnp.arange(peers, dtype=jnp.int32)
    sides = lax.axis_size("x")
    weights_at = ((x_at + sides - (step & (sides - 1))) & (sides - 1)) * 2 + (
        (c_at + step // sides) & 1
    )
    sign = 1 - 2 * (step & 1)
    block_at = (z_at + groups + sign * ((step + 1) // 2)) & (groups - 1)

    y_at, lane = lax.axis_index("y"), step[:lanes]
    turn, ahead = (y_at + lanes - lane) & (lanes - 1), (y_at + lane) & (lanes - 1)

    def gather_y(value):
        return tied(jnp.concatenate(gathered_turned(value, "y"), axis=0))

    def exchanged(value, axis):
        return lax.all_to_all(value, axis, split_axis=0, concat_axis=0, tiled=True)

    def along_y(value):
        return [value] + [shifted(value, "y", -s) for s in range(1, lanes)]

    r0 = gather_y(hidden_in)
    r0, w_gate_up, w_out, w_down = tied((r0, w_gate_up.transpose(1, 2, 0), w_out, w_down))
    f1, b1 = shifted(r0, "z", 1), shifted(r0, "z", -1)
    gates = gathered_turned(w_gate_up, "x")
    f2, b2 = shifted(f1, "z", 1), shifted(b1, "z", -1)
    downs = along_y(w_down)
    f3, b3 = shifted(f2, "z", 1), shifted(b2, "z", -1)
    w_heads = along_y(w_out)
    f4 = shifted(f3, "z", 1)
    first = qkv_first([r0, f1, b1, f2, b2], gain_attn, w_qkv)
    q, k, v = qkv_last(first, [f3, b3, f4], gain_attn, w_qkv)

    cache = cache_kv.reshape(seqs, spots, cache_kv.shape[3])
    seq_of = ((x_at + sides - step[:sides]) & (sides - 1)) // (sides // seqs)
    limits = jnp.where(seq_of == 0, cache_len[0], cache_len[1]) - kv_index * spots
    info = jnp.stack([seq_of, limits, (seq_of == x_at // (sides // seqs)).astype(jnp.int32)])
    q = lax.all_gather(q, "c", axis=0, tiled=True)
    queries = gathered_turned(q, "x")
    parts = list(attend((0,), info, queries[:1], k, v, cache))
    for slots in ((1, 3), (2,)):
        done = attend(slots, info, [queries[s] for s in slots], k, v, cache)
        parts += [shifted(part, "x", -s) for s, part in zip(slots, done)]
    downs = gathered_turned(jnp.stack(downs), "x")
    attended = combine(turn, exchanged(merge(parts, lax.axis_size("c")), "c"))

    attended, gates = tied((attended, gates))
    gates = jnp.stack(gates)
    gates = [gates, shifted(gates, "c", 1)]
    heads_here = exchanged(attended, "y")
    terms = project(block_at, ahead, heads_here, w_heads)
    terms = exchanged(terms, "z")
    residual, normed = add_and_norm(terms, hidden_in, gain_mlp)
    normed, gates = tied((normed, gates))

    r0 = gather_y(normed)
    f1, b1 = shifted(r0, "z", 1), shifted(r0, "z", -1)
    f2, b2 = shifted(f1, "z", 1), shifted(b1, "z", -1)
    f3, b3 = shifted(f2, "z", 1), shifted(b2, "z", -1)
    f3, b3, downs = tied((f3, b3, downs))
    downs = downs + [shifted(d, "c", 1) for d in downs]
    f4 = shifted(f3, "z", 1)
    first = gate_up(weights_at, [r0, f1, b1, f2, b2], gates)
    pieces = gate_up(weights_at, [f3, b3, f4], gates, turn, first)
    pieces = exchanged(pieces, "y")
    shares = exchanged(down(weights_at, block_at, ahead, pieces, downs), "z")
    return (residual + shares.astype(F32).sum(axis=0)).astype(BF16)


def solution(mesh):
    split = Mesh(mesh.devices.reshape(8, 4, 4, 2), ("z", "y", "x", "c"))
    in_specs = (
        P(KV_TP, None),
        P(),
        P(None, TP, None),
        P(None, KV, TP, None),
        P(),
        P(TP, None),
        P(),
        P(KV, None, TP),
        P(TP, KV),
    )
    return jax.shard_map(
        per_device, mesh=split, in_specs=in_specs, out_specs=P(KV_TP, None), check_vma=False
    )
```

```python
import functools
import math

import jax
import jax.numpy as jnp
from jax import lax
from jax.experimental import pallas as pl
from jax.experimental.pallas import tpu as pltpu
from jax.sharding import Mesh
from jax.sharding import PartitionSpec as P


TP = ("z", "y")
KV = ("x", "c")
KV_TP = ("x", "c", "z", "y")

EPSILON = 1e-05
MASKED = -1e30
LOG2E = 1.4426950408889634
F32 = jnp.float32
BF16 = jnp.bfloat16


def shifted(value, axis, step):
    count = lax.axis_size(axis)
    return lax.ppermute(value, axis, [(i, (i + step) % count) for i in range(count)])


def gathered_turned(value, axis):
    return [value] + [shifted(value, axis, s) for s in range(1, lax.axis_size(axis))]


def dot(a, b, ca, cb):
    return lax.dot_general(a, b, (((ca,), (cb,)), ((), ())), preferred_element_type=F32)


def run(kernel, table, arrays, outs, flops=0, limit=16):
    return pl.pallas_call(
        kernel,
        in_specs=[pl.BlockSpec(memory_space=pltpu.SMEM)]
        + [pl.BlockSpec(memory_space=pltpu.VMEM)] * len(arrays),
        out_specs=[pl.BlockSpec(memory_space=pltpu.VMEM)] * len(outs),
        out_shape=[jax.ShapeDtypeStruct(shape, kind) for shape, kind in outs],
        compiler_params=pltpu.CompilerParams(vmem_limit_bytes=limit << 20),
        cost_estimate=pl.CostEstimate(flops=flops, transcendentals=0, bytes_accessed=0),
    )(table, *arrays)


WEIGHTS, BLOCKS, TURN, AHEAD, SEQ, LIMIT, OWN, CORE = range(8)


def table_of_places(cache_len, seqs, spots):
    groups, lanes, sides = lax.axis_size("z"), lax.axis_size("y"), lax.axis_size("x")
    x_at, c_at, z_at, y_at = (lax.axis_index(name) for name in ("x", "c", "z", "y"))
    step = jnp.arange(8, dtype=jnp.int32)
    x_from = (x_at + 2 * sides - step) & (sides - 1)
    seq = x_from // (sides // seqs)
    rows = [None] * 8
    rows[WEIGHTS] = 2 * x_from + ((c_at + step // sides) & 1)
    rows[BLOCKS] = (z_at + groups + (1 - 2 * (step & 1)) * ((step + 1) // 2)) & (groups - 1)
    rows[TURN] = (y_at + 2 * lanes - step) & (lanes - 1)
    rows[AHEAD] = (y_at + step) & (lanes - 1)
    rows[SEQ] = seq
    rows[LIMIT] = jnp.where(seq == 0, cache_len[0], cache_len[1]) - (2 * x_at + c_at) * spots
    rows[OWN] = (seq == x_at // (sides // seqs)).astype(jnp.int32)
    rows[CORE] = c_at + 0 * step
    return jnp.stack(rows)


def rows_of(blocks):
    return sum(block.shape[0] for block in blocks)


def project_rows(x_refs, gain_ref, w_ref):
    steps = 4
    width = w_ref.shape[0] // steps
    scales = []
    for ref in x_refs:
        x = ref[...].astype(F32)
        scales.append(lax.rsqrt(jnp.mean(x * x, axis=1, keepdims=True) + EPSILON))

    def body(j, acc):
        cols = pl.ds(pl.multiple_of(j * width, width), width)
        gain = gain_ref[:, cols]
        normed = jnp.concatenate(
            [(ref[:, cols].astype(F32) * inv * gain) for ref, inv in zip(x_refs, scales)], axis=0
        ).astype(BF16)
        return acc + dot(normed, w_ref[cols], 1, 0)

    return lax.fori_loop(0, steps, body, jnp.zeros((rows_of(x_refs), w_ref.shape[1]), F32))


def qkv_first_kernel(table_ref, gain_ref, w_ref, *refs):
    *x_refs, out_ref = refs
    out_ref[...] = project_rows(x_refs, gain_ref, w_ref).astype(BF16)


def qkv_last_kernel(table_ref, gain_ref, w_ref, first_ref, *refs):
    *x_refs, q_ref, k_ref, v_ref = refs
    acc = project_rows(x_refs, gain_ref, w_ref).astype(BF16)
    size = q_ref.shape[1]
    done = first_ref.shape[0]
    for at, ref in enumerate((q_ref, k_ref, v_ref)):
        ref[:done] = first_ref[:, at * size : (at + 1) * size]
        ref[done:] = acc[:, at * size : (at + 1) * size]


def qkv_first(table, blocks, gain, weights):
    depth, packed = weights.shape
    count = rows_of(blocks)
    (out,) = run(
        qkv_first_kernel,
        table,
        [gain, weights, *blocks],
        [((count, packed), BF16)],
        2 * count * depth * packed,
    )
    return out


def qkv_last(table, first, blocks, gain, weights):
    depth, packed = weights.shape
    count = rows_of(blocks)
    return run(
        qkv_last_kernel,
        table,
        [gain, weights, first, *blocks],
        [((count + first.shape[0], packed // 3), BF16)] * 3,
        2 * count * depth * packed,
    )


def split3(value):
    first = value.astype(BF16).astype(F32)
    second = (value - first).astype(BF16).astype(F32)
    return first, second, value - first - second


def stats_of(peak, mass):
    row = lax.broadcasted_iota(jnp.int32, (16, peak.shape[1]), 0)
    stats = jnp.zeros((16, peak.shape[1]), F32)
    for at, part in enumerate(split3(peak) + split3(mass)):
        stats = jnp.where(row == at, part, stats)
    return stats.astype(BF16)


def attend_kernel(slots, table_ref, k_ref, v_ref, cache_ref, *refs):
    size = k_ref.shape[1]
    scale = LOG2E / math.sqrt(size)
    blocks = k_ref.shape[0]
    for q_ref, out_ref, slot in zip(refs[: len(slots)], refs[len(slots) :], slots):
        seq = table_ref[SEQ, slot]
        limit = table_ref[LIMIT, slot]
        own = table_ref[OWN, slot] > 0

        @pl.loop(0, q_ref.shape[0] // blocks)
        def _(part, q_ref=q_ref, out_ref=out_ref, seq=seq, limit=limit, own=own):
            at = pl.ds(pl.multiple_of(part * blocks, blocks), blocks)
            q = q_ref[at]
            s1 = dot(cache_ref[seq, :, :size], q, 1, 1) * scale
            s2 = dot(k_ref[...], q, 1, 1) * scale
            usable = lax.broadcasted_iota(jnp.int32, s1.shape, 0) < limit
            s1 = jnp.where(usable, s1, MASKED)
            s2 = jnp.where(own, s2, MASKED)
            top = jnp.maximum(jnp.max(s1, axis=0, keepdims=True), jnp.max(s2, axis=0, keepdims=True))
            peak = jnp.maximum(top, 0.1 * MASKED)
            p1 = jnp.exp2(s1 - peak)
            p2 = jnp.exp2(s2 - peak)
            mass = jnp.sum(p1, axis=0, keepdims=True) + jnp.sum(p2, axis=0, keepdims=True)
            acc = dot(cache_ref[seq, :, size:], p1.astype(BF16), 0, 0)
            acc += dot(v_ref[...], p2.astype(BF16), 0, 0)
            out_ref[:size, at] = acc.astype(BF16)
            out_ref[size:, at] = stats_of(peak, mass)


def attend(table, slots, queries, k, v, cache):
    count, size = k.shape
    return run(
        functools.partial(attend_kernel, slots),
        table,
        [k, v, cache, *queries],
        [((size + 16, q.shape[0]), BF16) for q in queries],
        4 * rows_of(queries) * size * (cache.shape[1] + count),
    )


def merged(parts, size):
    stats = [part[size:].astype(F32) for part in parts]
    peaks = [s[0:1] + s[1:2] + s[2:3] for s in stats]
    best = functools.reduce(jnp.maximum, peaks)
    mass = jnp.zeros_like(best)
    acc = jnp.zeros((size, best.shape[1]), F32)
    for part, s, peak in zip(parts, stats, peaks):
        scaling = jnp.exp2(peak - best)
        mass += (s[3:4] + s[4:5] + s[5:6]) * scaling
        acc += part[:size].astype(F32) * scaling
    return best, mass, acc


def merge_kernel(table_ref, *refs):
    *parts, mine_ref, other_ref = refs
    height, width = mine_ref.shape
    size = height - 16
    core = table_ref[CORE, 0]
    for ref, side in ((mine_ref, core), (other_ref, 1 - core)):
        cols = pl.ds(pl.multiple_of(side * width, width), width)
        best, mass, acc = merged([part[:, cols] for part in parts], size)
        ref[:size] = acc.astype(BF16)
        ref[size:] = stats_of(best, mass)


def merge(table, parts):
    height, width = parts[0].shape
    return run(merge_kernel, table, parts, [((height, width // 2), BF16)] * 2)


def combine_kernel(table_ref, mine_ref, other_ref, out_ref):
    size = mine_ref.shape[0] - 16
    lanes, rows, _ = out_ref.shape
    _, mass, acc = merged([mine_ref[...], other_ref[...]], size)
    attended = (acc / mass).T.reshape(rows // 8, lanes, 8, size)
    for s in range(lanes):
        out_ref[table_ref[TURN, s]] = attended[:, s].reshape(rows, size).astype(BF16)


def combine(table, mine, other, lanes):
    height, width = mine.shape
    shape = (lanes, width // lanes, height - 16)
    (out,) = run(combine_kernel, table, [mine, other], [(shape, BF16)])
    return out


def project_kernel(table_ref, heads_ref, *refs):
    *w_refs, out_ref = refs
    groups, rows, width = out_ref.shape
    heads = jnp.concatenate(
        [heads_ref[table_ref[AHEAD, s]] for s in range(len(w_refs))], axis=1
    )
    tile = width // 4

    @pl.loop(0, 4)
    def _(j):
        cols = pl.ds(pl.multiple_of(j * tile, tile), tile)
        acc = dot(heads, jnp.concatenate([w[:, cols] for w in w_refs], axis=0), 1, 0)
        acc = acc.reshape(groups, rows, tile)
        for s in range(groups):
            out_ref[table_ref[BLOCKS, s], :, cols] = acc[s].astype(BF16)


def project(table, heads, weights, groups):
    _, rows, _ = heads.shape
    shape = (groups, rows // groups, weights[0].shape[1])
    (out,) = run(project_kernel, table, [heads, *weights], [(shape, BF16)])
    return out


def residual_kernel(table_ref, terms_ref, hidden_ref, gain_ref, residual_ref, normed_ref):
    total = terms_ref[0].astype(F32)
    for s in range(1, terms_ref.shape[0]):
        total += terms_ref[s].astype(F32)
    total += hidden_ref[...].astype(F32)
    residual_ref[...] = total
    inv = lax.rsqrt(jnp.mean(total * total, axis=1, keepdims=True) + EPSILON)
    normed_ref[...] = (total * inv * gain_ref[...]).astype(BF16)


def add_and_norm(table, terms, hidden, gain):
    outs = [(hidden.shape, F32), (hidden.shape, BF16)]
    return run(residual_kernel, table, [terms, hidden, gain], outs)


def activated_rows(table_ref, x_refs, w_refs):
    side, _, hidden, depth = w_refs[0].shape
    gate = up = jnp.zeros((hidden, rows_of(x_refs)), F32)
    for at, w_ref in enumerate(w_refs):

        def body(j, sums, at=at, w_ref=w_ref):
            place = table_ref[WEIGHTS, at * side + j]
            cols = pl.ds(pl.multiple_of(place * depth, depth), depth)
            x = jnp.concatenate([ref[:, cols] for ref in x_refs], axis=0)
            gate, up = sums
            return gate + dot(w_ref[j, 0], x, 1, 1), up + dot(w_ref[j, 1], x, 1, 1)

        gate, up = lax.fori_loop(0, side, body, (gate, up))
    return (gate / (1.0 + jnp.exp(-gate)) * up).T


def gate_up_first_kernel(table_ref, near_ref, far_ref, *refs):
    *x_refs, out_ref = refs
    out_ref[...] = activated_rows(table_ref, x_refs, (near_ref, far_ref)).astype(BF16)


def gate_up_last_kernel(table_ref, near_ref, far_ref, first_ref, *refs):
    *x_refs, out_ref = refs
    done = first_ref.shape[0]
    out_ref[:done] = first_ref[...]
    out_ref[done:] = activated_rows(table_ref, x_refs, (near_ref, far_ref)).astype(BF16)


def gate_up(table, blocks, weights, first=None):
    count = rows_of(blocks)
    side, _, hidden, depth = weights[0].shape
    flops = 8 * count * side * hidden * depth
    if first is None:
        kernel, lead = gate_up_first_kernel, []
    else:
        kernel, lead = gate_up_last_kernel, [first]
    shape = (count + rows_of(lead), hidden)
    (out,) = run(kernel, table, [*weights, *lead, *blocks], [(shape, BF16)], flops)
    return out


def down_kernel(lanes, table_ref, x_ref, *refs):
    w_refs, out_refs = refs[:-lanes], refs[-lanes:]
    rows, side, width = x_ref.shape[0], w_refs[0].shape[0], w_refs[0].shape[2]
    for at, w_ref in enumerate(w_refs):

        @pl.loop(0, side)
        def _(j, at=at, w_ref=w_ref):
            acc = dot(x_ref[...], w_ref[j], 1, 0).reshape(rows // (8 * lanes), lanes, 8, width)
            place = table_ref[WEIGHTS, at * side + j]
            cols = pl.ds(pl.multiple_of(place * width, width), width)
            for s, ref in enumerate(out_refs):
                ref[:, cols] = acc[:, s].reshape(rows // lanes, width).astype(BF16)


def down(table, rows, weights, lanes):
    side, _, width = weights[0].shape
    shape = (rows.shape[0] // lanes, side * width * len(weights))
    return run(
        functools.partial(down_kernel, lanes), table, [rows, *weights], [(shape, BF16)] * lanes
    )


def sum_kernel(table_ref, *refs):
    *ins, out_ref = refs
    total = ins[0][...].astype(F32)
    for ref in ins[1:]:
        total += ref[...].astype(F32)
    groups, rows, width = out_ref.shape
    total = total.reshape(groups, rows, width)
    for s in range(groups):
        out_ref[table_ref[BLOCKS, s]] = total[s].astype(BF16)


def sum_pieces(table, pieces, groups):
    rows, width = pieces[0].shape
    outs = [((groups, rows // groups, width), BF16)]
    (out,) = run(sum_kernel, table, pieces, outs)
    return out


def per_device(
    hidden_in, gain_attn, w_qkv, cache_kv, cache_len, w_out, gain_mlp, w_gate_up, w_down
):
    depth, _, packed = w_qkv.shape
    seqs, spots = cache_kv.shape[:2]
    groups, lanes = lax.axis_size("z"), lax.axis_size("y")
    tied = lax.optimization_barrier
    w_qkv = w_qkv.reshape(depth, packed)
    gain_attn, gain_mlp = gain_attn.reshape(1, depth), gain_mlp.reshape(1, depth)
    cache = cache_kv.reshape(seqs, spots, cache_kv.shape[3])
    table = table_of_places(cache_len, seqs, spots)

    def gather_y(value):
        return tied(jnp.concatenate(gathered_turned(value, "y"), axis=0))

    def along_y(value):
        return [value] + [shifted(value, "y", -s) for s in range(1, lanes)]

    def exchanged(value, axis):
        return lax.all_to_all(value, axis, split_axis=0, concat_axis=0, tiled=True)

    r0 = gather_y(hidden_in)
    r0, w_gate_up, w_out, w_down = tied((r0, w_gate_up.transpose(1, 2, 0), w_out, w_down))
    f1, b1 = shifted(r0, "z", 1), shifted(r0, "z", -1)
    gates = gathered_turned(w_gate_up, "x")
    f2, b2 = shifted(f1, "z", 1), shifted(b1, "z", -1)
    w_heads = along_y(w_out)
    f3, b3 = shifted(f2, "z", 1), shifted(b2, "z", -1)
    f4 = shifted(f3, "z", 1)
    first = qkv_first(table, [r0, f1, b1, f2, b2], gain_attn, w_qkv)
    q, k, v = qkv_last(table, first, [f3, b3, f4], gain_attn, w_qkv)

    q = lax.all_gather(q, "c", axis=0, tiled=True)
    queries = gathered_turned(q, "x")
    parts = list(attend(table, (0,), queries[:1], k, v, cache))
    for slots in ((1, 3), (2,)):
        done = attend(table, slots, [queries[s] for s in slots], k, v, cache)
        parts += [shifted(part, "x", -s) for s, part in zip(slots, done)]
    mine, other = merge(table, parts)
    other = shifted(other, "c", 1)
    attended = combine(table, mine, other, lanes)

    attended, gates = tied((attended, gates))
    gates = jnp.stack(gates)
    gates = [gates, shifted(gates, "c", 1)]
    heads_here = exchanged(attended, "y")
    terms = project(table, heads_here, w_heads, groups)
    downs = gathered_turned(w_down, "x")
    terms = exchanged(terms, "z")
    residual, normed = add_and_norm(table, terms, hidden_in, gain_mlp)
    normed, gates = tied((normed, gates))

    r0 = gather_y(normed)
    f1, b1 = shifted(r0, "z", 1), shifted(r0, "z", -1)
    f2, b2 = shifted(f1, "z", 1), shifted(b1, "z", -1)
    f3, b3 = shifted(f2, "z", 1), shifted(b2, "z", -1)
    downs = jnp.stack(downs)
    downs = [downs, shifted(downs, "c", 1)]
    f4 = shifted(f3, "z", 1)
    first = gate_up(table, [r0, f1, b1, f2, b2], gates)
    activated = gate_up(table, [f3, b3, f4], gates, first)
    pieces = down(table, activated, downs, lanes)
    pieces = [shifted(piece, "y", -s) if s else piece for s, piece in enumerate(pieces)]
    shares = exchanged(sum_pieces(table, pieces, groups), "z")
    return (residual + shares.astype(F32).sum(axis=0)).astype(BF16)


def solution(mesh):
    split = Mesh(mesh.devices.reshape(8, 4, 4, 2), ("z", "y", "x", "c"))
    in_specs = (
        P(KV_TP, None),
        P(),
        P(None, TP, None),
        P(None, KV, TP, None),
        P(),
        P(TP, None),
        P(),
        P(KV, None, TP),
        P(TP, KV),
    )
    return jax.shard_map(
        per_device, mesh=split, in_specs=in_specs, out_specs=P(KV_TP, None), check_vma=False
    )
```

```python
import functools
import math

import jax
import jax.numpy as jnp
from jax import lax
from jax.experimental import pallas as pl
from jax.experimental.pallas import tpu as pltpu
from jax.sharding import Mesh
from jax.sharding import PartitionSpec as P


TP = ("z", "y")
KV = ("x", "c")
KV_TP = ("x", "c", "z", "y")

EPSILON = 1e-05
MASKED = -1e30
LOG2E = 1.4426950408889634
F32 = jnp.float32
BF16 = jnp.bfloat16


def shifted(value, axis, step):
    count = lax.axis_size(axis)
    return lax.ppermute(value, axis, [(i, (i + step) % count) for i in range(count)])


def gathered_turned(value, axis):
    return [value] + [shifted(value, axis, s) for s in range(1, lax.axis_size(axis))]


def dot(a, b, ca, cb):
    return lax.dot_general(a, b, (((ca,), (cb,)), ((), ())), preferred_element_type=F32)


def run(kernel, table, arrays, outs, flops=0, limit=16):
    return pl.pallas_call(
        kernel,
        in_specs=[pl.BlockSpec(memory_space=pltpu.SMEM)]
        + [pl.BlockSpec(memory_space=pltpu.VMEM)] * len(arrays),
        out_specs=[pl.BlockSpec(memory_space=pltpu.VMEM)] * len(outs),
        out_shape=[jax.ShapeDtypeStruct(shape, kind) for shape, kind in outs],
        compiler_params=pltpu.CompilerParams(vmem_limit_bytes=limit << 20),
        cost_estimate=pl.CostEstimate(flops=flops, transcendentals=0, bytes_accessed=0),
    )(table, *arrays)


WEIGHTS, BLOCKS, TURN, AHEAD, SEQ, LIMIT, OWN, CORE = range(8)


def table_of_places(cache_len, seqs, spots):
    groups, lanes, sides = lax.axis_size("z"), lax.axis_size("y"), lax.axis_size("x")
    x_at, c_at, z_at, y_at = (lax.axis_index(name) for name in ("x", "c", "z", "y"))
    step = jnp.arange(8, dtype=jnp.int32)
    x_from = (x_at + 2 * sides - step) & (sides - 1)
    seq = x_from // (sides // seqs)
    rows = [None] * 8
    rows[WEIGHTS] = 2 * x_from + ((c_at + step // sides) & 1)
    rows[BLOCKS] = (z_at + groups + (1 - 2 * (step & 1)) * ((step + 1) // 2)) & (groups - 1)
    rows[TURN] = (y_at + 2 * lanes - step) & (lanes - 1)
    rows[AHEAD] = (y_at + step) & (lanes - 1)
    rows[SEQ] = seq
    rows[LIMIT] = jnp.where(seq == 0, cache_len[0], cache_len[1]) - (2 * x_at + c_at) * spots
    rows[OWN] = (seq == x_at // (sides // seqs)).astype(jnp.int32)
    rows[CORE] = c_at + 0 * step
    return jnp.stack(rows)


def rows_of(blocks):
    return sum(block.shape[0] for block in blocks)


def project_rows(x_refs, gain_ref, w_ref):
    steps = 4
    width = w_ref.shape[0] // steps
    scales = []
    for ref in x_refs:
        x = ref[...].astype(F32)
        scales.append(lax.rsqrt(jnp.mean(x * x, axis=1, keepdims=True) + EPSILON))

    def body(j, acc):
        cols = pl.ds(pl.multiple_of(j * width, width), width)
        gain = gain_ref[:, cols]
        normed = jnp.concatenate(
            [(ref[:, cols].astype(F32) * inv * gain) for ref, inv in zip(x_refs, scales)], axis=0
        ).astype(BF16)
        return acc + dot(normed, w_ref[cols], 1, 0)

    return lax.fori_loop(0, steps, body, jnp.zeros((rows_of(x_refs), w_ref.shape[1]), F32))


def qkv_first_kernel(table_ref, gain_ref, w_ref, *refs):
    *x_refs, out_ref = refs
    out_ref[...] = project_rows(x_refs, gain_ref, w_ref).astype(BF16)


def qkv_last_kernel(table_ref, gain_ref, w_ref, first_ref, *refs):
    *x_refs, q_ref, k_ref, v_ref = refs
    acc = project_rows(x_refs, gain_ref, w_ref).astype(BF16)
    size = q_ref.shape[1]
    done = first_ref.shape[0]
    for at, ref in enumerate((q_ref, k_ref, v_ref)):
        ref[:done] = first_ref[:, at * size : (at + 1) * size]
        ref[done:] = acc[:, at * size : (at + 1) * size]


def qkv_first(table, blocks, gain, weights):
    depth, packed = weights.shape
    count = rows_of(blocks)
    (out,) = run(
        qkv_first_kernel,
        table,
        [gain, weights, *blocks],
        [((count, packed), BF16)],
        2 * count * depth * packed,
    )
    return out


def qkv_last(table, first, blocks, gain, weights):
    depth, packed = weights.shape
    count = rows_of(blocks)
    return run(
        qkv_last_kernel,
        table,
        [gain, weights, first, *blocks],
        [((count + first.shape[0], packed // 3), BF16)] * 3,
        2 * count * depth * packed,
    )


def split3(value):
    first = value.astype(BF16).astype(F32)
    second = (value - first).astype(BF16).astype(F32)
    return first, second, value - first - second


def stats_of(peak, mass):
    row = lax.broadcasted_iota(jnp.int32, (16, peak.shape[1]), 0)
    stats = jnp.zeros((16, peak.shape[1]), F32)
    for at, part in enumerate(split3(peak) + split3(mass)):
        stats = jnp.where(row == at, part, stats)
    return stats.astype(BF16)


def attend_kernel(slots, table_ref, k_ref, v_ref, cache_ref, *refs):
    size = k_ref.shape[1]
    scale = LOG2E / math.sqrt(size)
    blocks = k_ref.shape[0]
    for q_ref, out_ref, slot in zip(refs[: len(slots)], refs[len(slots) :], slots):
        seq = table_ref[SEQ, slot]
        limit = table_ref[LIMIT, slot]
        own = table_ref[OWN, slot] > 0

        @pl.loop(0, q_ref.shape[0] // blocks)
        def _(part, q_ref=q_ref, out_ref=out_ref, seq=seq, limit=limit, own=own):
            at = pl.ds(pl.multiple_of(part * blocks, blocks), blocks)
            q = q_ref[at]
            s1 = dot(cache_ref[seq, :, :size], q, 1, 1) * scale
            s2 = dot(k_ref[...], q, 1, 1) * scale
            usable = lax.broadcasted_iota(jnp.int32, s1.shape, 0) < limit
            s1 = jnp.where(usable, s1, MASKED)
            s2 = jnp.where(own, s2, MASKED)
            top = jnp.maximum(jnp.max(s1, axis=0, keepdims=True), jnp.max(s2, axis=0, keepdims=True))
            peak = jnp.maximum(top, 0.1 * MASKED)
            p1 = jnp.exp2(s1 - peak)
            p2 = jnp.exp2(s2 - peak)
            mass = jnp.sum(p1, axis=0, keepdims=True) + jnp.sum(p2, axis=0, keepdims=True)
            acc = dot(cache_ref[seq, :, size:], p1.astype(BF16), 0, 0)
            acc += dot(v_ref[...], p2.astype(BF16), 0, 0)
            out_ref[:size, at] = acc.astype(BF16)
            out_ref[size:, at] = stats_of(peak, mass)


def attend(table, slots, queries, k, v, cache):
    count, size = k.shape
    return run(
        functools.partial(attend_kernel, slots),
        table,
        [k, v, cache, *queries],
        [((size + 16, q.shape[0]), BF16) for q in queries],
        4 * rows_of(queries) * size * (cache.shape[1] + count),
    )


def merged(parts, size):
    stats = [part[size:].astype(F32) for part in parts]
    peaks = [s[0:1] + s[1:2] + s[2:3] for s in stats]
    best = functools.reduce(jnp.maximum, peaks)
    mass = jnp.zeros_like(best)
    acc = jnp.zeros((size, best.shape[1]), F32)
    for part, s, peak in zip(parts, stats, peaks):
        scaling = jnp.exp2(peak - best)
        mass += (s[3:4] + s[4:5] + s[5:6]) * scaling
        acc += part[:size].astype(F32) * scaling
    return best, mass, acc


def merge_kernel(table_ref, *refs):
    *parts, mine_ref, other_ref = refs
    height, width = mine_ref.shape
    size = height - 16
    core = table_ref[CORE, 0]
    for ref, side in ((mine_ref, core), (other_ref, 1 - core)):
        cols = pl.ds(pl.multiple_of(side * width, width), width)
        best, mass, acc = merged([part[:, cols] for part in parts], size)
        ref[:size] = acc.astype(BF16)
        ref[size:] = stats_of(best, mass)


def merge(table, parts):
    height, width = parts[0].shape
    return run(merge_kernel, table, parts, [((height, width // 2), BF16)] * 2)


def combine_kernel(table_ref, mine_ref, other_ref, out_ref):
    size = mine_ref.shape[0] - 16
    lanes, rows, _ = out_ref.shape
    _, mass, acc = merged([mine_ref[...], other_ref[...]], size)
    attended = (acc / mass).T.reshape(rows // 8, lanes, 8, size)
    for s in range(lanes):
        out_ref[table_ref[TURN, s]] = attended[:, s].reshape(rows, size).astype(BF16)


def combine(table, mine, other, lanes):
    height, width = mine.shape
    shape = (lanes, width // lanes, height - 16)
    (out,) = run(combine_kernel, table, [mine, other], [(shape, BF16)])
    return out


def project_kernel(table_ref, heads_ref, *refs):
    *w_refs, out_ref = refs
    groups, rows, width = out_ref.shape
    heads = jnp.concatenate(
        [heads_ref[table_ref[AHEAD, s]] for s in range(len(w_refs))], axis=1
    )
    tile = width // 4

    @pl.loop(0, 4)
    def _(j):
        cols = pl.ds(pl.multiple_of(j * tile, tile), tile)
        acc = dot(heads, jnp.concatenate([w[:, cols] for w in w_refs], axis=0), 1, 0)
        acc = acc.reshape(groups, rows, tile)
        for s in range(groups):
            out_ref[table_ref[BLOCKS, s], :, cols] = acc[s].astype(BF16)


def project(table, heads, weights, groups):
    _, rows, _ = heads.shape
    shape = (groups, rows // groups, weights[0].shape[1])
    (out,) = run(project_kernel, table, [heads, *weights], [(shape, BF16)])
    return out


def residual_kernel(table_ref, terms_ref, hidden_ref, gain_ref, residual_ref, normed_ref):
    total = terms_ref[0].astype(F32)
    for s in range(1, terms_ref.shape[0]):
        total += terms_ref[s].astype(F32)
    total += hidden_ref[...].astype(F32)
    residual_ref[...] = total
    inv = lax.rsqrt(jnp.mean(total * total, axis=1, keepdims=True) + EPSILON)
    normed_ref[...] = (total * inv * gain_ref[...]).astype(BF16)


def add_and_norm(table, terms, hidden, gain):
    outs = [(hidden.shape, F32), (hidden.shape, BF16)]
    return run(residual_kernel, table, [terms, hidden, gain], outs)


def activated_rows(table_ref, x_refs, w_refs):
    side, _, hidden, depth = w_refs[0].shape
    gate = up = jnp.zeros((hidden, rows_of(x_refs)), F32)
    for at, w_ref in enumerate(w_refs):

        def body(j, sums, at=at, w_ref=w_ref):
            place = table_ref[WEIGHTS, at * side + j]
            cols = pl.ds(pl.multiple_of(place * depth, depth), depth)
            x = jnp.concatenate([ref[:, cols] for ref in x_refs], axis=0)
            gate, up = sums
            return gate + dot(w_ref[j, 0], x, 1, 1), up + dot(w_ref[j, 1], x, 1, 1)

        gate, up = lax.fori_loop(0, side, body, (gate, up))
    return (gate / (1.0 + jnp.exp(-gate)) * up).T


def gate_up_first_kernel(table_ref, near_ref, far_ref, *refs):
    *x_refs, out_ref = refs
    out_ref[...] = activated_rows(table_ref, x_refs, (near_ref, far_ref)).astype(BF16)


def gate_up_last_kernel(table_ref, near_ref, far_ref, first_ref, *refs):
    *x_refs, out_ref = refs
    done = first_ref.shape[0]
    out_ref[:done] = first_ref[...]
    out_ref[done:] = activated_rows(table_ref, x_refs, (near_ref, far_ref)).astype(BF16)


def gate_up(table, blocks, weights, first=None):
    count = rows_of(blocks)
    side, _, hidden, depth = weights[0].shape
    flops = 8 * count * side * hidden * depth
    if first is None:
        kernel, lead = gate_up_first_kernel, []
    else:
        kernel, lead = gate_up_last_kernel, [first]
    shape = (count + rows_of(lead), hidden)
    (out,) = run(kernel, table, [*weights, *lead, *blocks], [(shape, BF16)], flops)
    return out


def down_kernel(lanes, table_ref, x_ref, *refs):
    w_refs, out_refs = refs[:-lanes], refs[-lanes:]
    rows, side, width = x_ref.shape[0], w_refs[0].shape[0], w_refs[0].shape[3]
    for at, w_ref in enumerate(w_refs):

        @pl.loop(0, side)
        def _(j, at=at, w_ref=w_ref):
            acc = dot(x_ref[...], w_ref[j, 2], 1, 0).reshape(rows // (8 * lanes), lanes, 8, width)
            place = table_ref[WEIGHTS, at * side + j]
            cols = pl.ds(pl.multiple_of(place * width, width), width)
            for s, ref in enumerate(out_refs):
                ref[:, cols] = acc[:, s].reshape(rows // lanes, width).astype(BF16)


def down(table, rows, weights, lanes):
    side, _, _, width = weights[0].shape
    shape = (rows.shape[0] // lanes, side * width * len(weights))
    return run(
        functools.partial(down_kernel, lanes), table, [rows, *weights], [(shape, BF16)] * lanes
    )


def sum_kernel(table_ref, *refs):
    *ins, out_ref = refs
    total = ins[0][...].astype(F32)
    for ref in ins[1:]:
        total += ref[...].astype(F32)
    groups, rows, width = out_ref.shape
    total = total.reshape(groups, rows, width)
    for s in range(groups):
        out_ref[table_ref[BLOCKS, s]] = total[s].astype(BF16)


def sum_pieces(table, pieces, groups):
    rows, width = pieces[0].shape
    outs = [((groups, rows // groups, width), BF16)]
    (out,) = run(sum_kernel, table, pieces, outs)
    return out


def per_device(
    hidden_in, gain_attn, w_qkv, cache_kv, cache_len, w_out, gain_mlp, w_gate_up, w_down
):
    depth, _, packed = w_qkv.shape
    seqs, spots = cache_kv.shape[:2]
    groups, lanes = lax.axis_size("z"), lax.axis_size("y")
    tied = lax.optimization_barrier
    w_qkv = w_qkv.reshape(depth, packed)
    gain_attn, gain_mlp = gain_attn.reshape(1, depth), gain_mlp.reshape(1, depth)
    cache = cache_kv.reshape(seqs, spots, cache_kv.shape[3])
    table = table_of_places(cache_len, seqs, spots)

    def gather_y(value):
        return tied(jnp.concatenate(gathered_turned(value, "y"), axis=0))

    def along_y(value):
        return [value] + [shifted(value, "y", -s) for s in range(1, lanes)]

    def exchanged(value, axis):
        return lax.all_to_all(value, axis, split_axis=0, concat_axis=0, tiled=True)

    w_mlp = jnp.concatenate([w_gate_up.transpose(1, 2, 0), w_down[None]], axis=0)
    r0 = gather_y(hidden_in)
    w_mlp = gathered_turned(w_mlp, "x")
    f1, b1 = shifted(r0, "z", 1), shifted(r0, "z", -1)
    f2, b2 = shifted(f1, "z", 1), shifted(b1, "z", -1)
    w_heads = along_y(w_out)
    f3, b3 = shifted(f2, "z", 1), shifted(b2, "z", -1)
    f4 = shifted(f3, "z", 1)
    first = qkv_first(table, [r0, f1, b1, f2, b2], gain_attn, w_qkv)
    q, k, v = qkv_last(table, first, [f3, b3, f4], gain_attn, w_qkv)

    q = lax.all_gather(q, "c", axis=0, tiled=True)
    queries = gathered_turned(q, "x")
    parts = list(attend(table, (0,), queries[:1], k, v, cache))
    for slots in ((1, 3), (2,)):
        done = attend(table, slots, [queries[s] for s in slots], k, v, cache)
        parts += [shifted(part, "x", -s) for s, part in zip(slots, done)]
    mine, other = merge(table, parts)
    other = shifted(other, "c", 1)
    attended = combine(table, mine, other, lanes)

    w_mlp = jnp.stack(w_mlp)
    w_mlp = [w_mlp, shifted(w_mlp, "c", 1)]
    heads_here = exchanged(attended, "y")
    terms = project(table, heads_here, w_heads, groups)
    terms = exchanged(terms, "z")
    residual, normed = add_and_norm(table, terms, hidden_in, gain_mlp)
    r0 = gather_y(normed)
    f1, b1 = shifted(r0, "z", 1), shifted(r0, "z", -1)
    f2, b2 = shifted(f1, "z", 1), shifted(b1, "z", -1)
    f3, b3 = shifted(f2, "z", 1), shifted(b2, "z", -1)
    f4 = shifted(f3, "z", 1)
    first = gate_up(table, [r0, f1, b1, f2, b2], w_mlp)
    activated = gate_up(table, [f3, b3, f4], w_mlp, first)
    pieces = down(table, activated, w_mlp, lanes)
    pieces = [shifted(piece, "y", -s) if s else piece for s, piece in enumerate(pieces)]
    shares = exchanged(sum_pieces(table, pieces, groups), "z")
    return (residual + shares.astype(F32).sum(axis=0)).astype(BF16)


def solution(mesh):
    split = Mesh(mesh.devices.reshape(8, 4, 4, 2), ("z", "y", "x", "c"))
    in_specs = (
        P(KV_TP, None),
        P(),
        P(None, TP, None),
        P(None, KV, TP, None),
        P(),
        P(TP, None),
        P(),
        P(KV, None, TP),
        P(TP, KV),
    )
    return jax.shard_map(
        per_device, mesh=split, in_specs=in_specs, out_specs=P(KV_TP, None), check_vma=False
    )
```

```python
import functools
import math

import jax
import jax.numpy as jnp
from jax import lax
from jax.experimental import pallas as pl
from jax.experimental.pallas import tpu as pltpu
from jax.sharding import Mesh
from jax.sharding import PartitionSpec as P


TP = ("z", "y")
KV = ("x", "c")
KV_TP = ("x", "c", "z", "y")

EPSILON = 1e-05
MASKED = -1e30
LOG2E = 1.4426950408889634
F32 = jnp.float32
BF16 = jnp.bfloat16


def shifted(value, axis, step):
    count = lax.axis_size(axis)
    return lax.ppermute(value, axis, [(i, (i + step) % count) for i in range(count)])


def gathered_turned(value, axis):
    return [value] + [shifted(value, axis, s) for s in range(1, lax.axis_size(axis))]


def dot(a, b, ca, cb):
    return lax.dot_general(a, b, (((ca,), (cb,)), ((), ())), preferred_element_type=F32)


def run(kernel, table, arrays, outs, flops=0, limit=16, scratch=()):
    return pl.pallas_call(
        kernel,
        in_specs=[pl.BlockSpec(memory_space=pltpu.SMEM)]
        + [pl.BlockSpec(memory_space=pltpu.VMEM)] * len(arrays),
        out_specs=[pl.BlockSpec(memory_space=pltpu.VMEM)] * len(outs),
        out_shape=[jax.ShapeDtypeStruct(shape, kind) for shape, kind in outs],
        scratch_shapes=[pltpu.VMEM(shape, kind) for shape, kind in scratch],
        compiler_params=pltpu.CompilerParams(vmem_limit_bytes=limit << 20),
        cost_estimate=pl.CostEstimate(flops=flops, transcendentals=0, bytes_accessed=0),
    )(table, *arrays)


WEIGHTS, BLOCKS, TURN, AHEAD, SEQ, LIMIT, OWN, CORE = range(8)


def table_of_places(cache_len, seqs, spots):
    groups, lanes, sides = lax.axis_size("z"), lax.axis_size("y"), lax.axis_size("x")
    x_at, c_at, z_at, y_at = (lax.axis_index(name) for name in ("x", "c", "z", "y"))
    step = jnp.arange(8, dtype=jnp.int32)
    x_from = (x_at + 2 * sides - step) & (sides - 1)
    seq = x_from // (sides // seqs)
    rows = [None] * 8
    rows[WEIGHTS] = 2 * x_from + ((c_at + step // sides) & 1)
    rows[BLOCKS] = (z_at + groups + (1 - 2 * (step & 1)) * ((step + 1) // 2)) & (groups - 1)
    rows[TURN] = (y_at + 2 * lanes - step) & (lanes - 1)
    rows[AHEAD] = (y_at + step) & (lanes - 1)
    rows[SEQ] = seq
    rows[LIMIT] = jnp.where(seq == 0, cache_len[0], cache_len[1]) - (2 * x_at + c_at) * spots
    rows[OWN] = (seq == x_at // (sides // seqs)).astype(jnp.int32)
    rows[CORE] = c_at + 0 * step
    return jnp.stack(rows)


def rows_of(blocks):
    return sum(block.shape[0] for block in blocks)


def project_rows(x_refs, gain_ref, w_ref):
    steps = 4
    width = w_ref.shape[0] // steps

    def chunk(j):
        cols = pl.ds(pl.multiple_of(j * width, width), width)
        return cols, jnp.concatenate([ref[:, cols] for ref in x_refs], axis=0).astype(F32)

    def squares(j, total):
        _, x = chunk(j)
        return total + jnp.sum(x * x, axis=1, keepdims=True)

    total = lax.fori_loop(0, steps, squares, jnp.zeros((rows_of(x_refs), 1), F32))
    inv = lax.rsqrt(total / w_ref.shape[0] + EPSILON)

    def body(j, acc):
        cols, x = chunk(j)
        return acc + dot((x * inv * gain_ref[:, cols]).astype(BF16), w_ref[cols], 1, 0)

    return lax.fori_loop(0, steps, body, jnp.zeros((rows_of(x_refs), w_ref.shape[1]), F32))


def qkv_first_kernel(table_ref, gain_ref, w_ref, *refs):
    *x_refs, out_ref = refs
    out_ref[...] = project_rows(x_refs, gain_ref, w_ref).astype(BF16)


def qkv_last_kernel(table_ref, gain_ref, w_ref, first_ref, *refs):
    *x_refs, q_ref, k_ref, v_ref = refs
    acc = project_rows(x_refs, gain_ref, w_ref).astype(BF16)
    size = q_ref.shape[1]
    done = first_ref.shape[0]
    for at, ref in enumerate((q_ref, k_ref, v_ref)):
        ref[:done] = first_ref[:, at * size : (at + 1) * size]
        ref[done:] = acc[:, at * size : (at + 1) * size]


def qkv_first(table, blocks, gain, weights):
    depth, packed = weights.shape
    count = rows_of(blocks)
    (out,) = run(
        qkv_first_kernel,
        table,
        [gain, weights, *blocks],
        [((count, packed), BF16)],
        2 * count * depth * packed,
    )
    return out


def qkv_last(table, first, blocks, gain, weights):
    depth, packed = weights.shape
    count = rows_of(blocks)
    return run(
        qkv_last_kernel,
        table,
        [gain, weights, first, *blocks],
        [((count + first.shape[0], packed // 3), BF16)] * 3,
        2 * count * depth * packed,
    )


def split3(value):
    first = value.astype(BF16).astype(F32)
    second = (value - first).astype(BF16).astype(F32)
    return first, second, value - first - second


def stats_of(peak, mass):
    row = lax.broadcasted_iota(jnp.int32, (16, peak.shape[1]), 0)
    stats = jnp.zeros((16, peak.shape[1]), F32)
    for at, part in enumerate(split3(peak) + split3(mass)):
        stats = jnp.where(row == at, part, stats)
    return stats.astype(BF16)


def attend_kernel(slots, table_ref, k_ref, v_ref, cache_ref, *refs):
    *refs, q_buf, out_buf = refs
    q_refs, out_refs = refs[: len(slots)], refs[len(slots) :]
    blocks, size = k_ref.shape
    scale = LOG2E / math.sqrt(size)
    halves = q_buf.shape[1] // blocks
    for at, ref in enumerate(q_refs):
        q_buf[at] = ref[...]

    @pl.loop(0, len(slots) * halves)
    def _(turn):
        which, half = turn // halves, turn % halves
        slot = slots[0] + which * (slots[-1] - slots[0])
        seq = table_ref[SEQ, slot]
        limit = table_ref[LIMIT, slot]
        own = table_ref[OWN, slot] > 0
        at = pl.ds(pl.multiple_of(half * blocks, blocks), blocks)
        q = q_buf[which, at]
        s1 = dot(cache_ref[seq, :, :size], q, 1, 1) * scale
        s2 = dot(k_ref[...], q, 1, 1) * scale
        usable = lax.broadcasted_iota(jnp.int32, s1.shape, 0) < limit
        s1 = jnp.where(usable, s1, MASKED)
        s2 = jnp.where(own, s2, MASKED)
        top = jnp.maximum(jnp.max(s1, axis=0, keepdims=True), jnp.max(s2, axis=0, keepdims=True))
        peak = jnp.maximum(top, 0.1 * MASKED)
        p1 = jnp.exp2(s1 - peak)
        p2 = jnp.exp2(s2 - peak)
        mass = jnp.sum(p1, axis=0, keepdims=True) + jnp.sum(p2, axis=0, keepdims=True)
        acc = dot(cache_ref[seq, :, size:], p1.astype(BF16), 0, 0)
        acc += dot(v_ref[...], p2.astype(BF16), 0, 0)
        out_buf[which, :size, at] = acc.astype(BF16)
        out_buf[which, size:, at] = stats_of(peak, mass)

    for at, ref in enumerate(out_refs):
        ref[...] = out_buf[at]


def attend(table, slots, queries, k, v, cache):
    count, size = k.shape
    rows = queries[0].shape[0]
    return run(
        functools.partial(attend_kernel, slots),
        table,
        [k, v, cache, *queries],
        [((size + 16, rows), BF16)] * len(slots),
        4 * rows_of(queries) * size * (cache.shape[1] + count),
        scratch=[((len(slots), rows, size), BF16), ((len(slots), size + 16, rows), BF16)],
    )


def merged(parts, size):
    stats = [part[size:].astype(F32) for part in parts]
    peaks = [s[0:1] + s[1:2] + s[2:3] for s in stats]
    best = functools.reduce(jnp.maximum, peaks)
    mass = jnp.zeros_like(best)
    acc = jnp.zeros((size, best.shape[1]), F32)
    for part, s, peak in zip(parts, stats, peaks):
        scaling = jnp.exp2(peak - best)
        mass += (s[3:4] + s[4:5] + s[5:6]) * scaling
        acc += part[:size].astype(F32) * scaling
    return best, mass, acc


def merge_kernel(table_ref, *refs):
    *parts, mine_ref, other_ref = refs
    height, width = mine_ref.shape
    size = height - 16
    core = table_ref[CORE, 0]
    for ref, side in ((mine_ref, core), (other_ref, 1 - core)):
        cols = pl.ds(pl.multiple_of(side * width, width), width)
        best, mass, acc = merged([part[:, cols] for part in parts], size)
        ref[:size] = acc.astype(BF16)
        ref[size:] = stats_of(best, mass)


def merge(table, parts):
    height, width = parts[0].shape
    return run(merge_kernel, table, parts, [((height, width // 2), BF16)] * 2)


def combine_kernel(table_ref, mine_ref, other_ref, out_ref):
    size = mine_ref.shape[0] - 16
    lanes, rows, _ = out_ref.shape
    _, mass, acc = merged([mine_ref[...], other_ref[...]], size)
    attended = (acc / mass).T.reshape(rows // 8, lanes, 8, size)
    for s in range(lanes):
        out_ref[table_ref[TURN, s]] = attended[:, s].reshape(rows, size).astype(BF16)


def combine(table, mine, other, lanes):
    height, width = mine.shape
    shape = (lanes, width // lanes, height - 16)
    (out,) = run(combine_kernel, table, [mine, other], [(shape, BF16)])
    return out


def project_kernel(table_ref, heads_ref, *refs):
    *w_refs, out_ref = refs
    groups, rows, width = out_ref.shape
    heads = jnp.concatenate(
        [heads_ref[table_ref[AHEAD, s]] for s in range(len(w_refs))], axis=1
    )
    tile = width // 4

    @pl.loop(0, 4)
    def _(j):
        cols = pl.ds(pl.multiple_of(j * tile, tile), tile)
        acc = dot(heads, jnp.concatenate([w[:, cols] for w in w_refs], axis=0), 1, 0)
        acc = acc.reshape(groups, rows, tile)
        for s in range(groups):
            out_ref[table_ref[BLOCKS, s], :, cols] = acc[s].astype(BF16)


def project(table, heads, weights, groups):
    _, rows, _ = heads.shape
    shape = (groups, rows // groups, weights[0].shape[1])
    (out,) = run(project_kernel, table, [heads, *weights], [(shape, BF16)])
    return out


def residual_kernel(table_ref, terms_ref, hidden_ref, gain_ref, residual_ref, normed_ref):
    total = terms_ref[0].astype(F32)
    for s in range(1, terms_ref.shape[0]):
        total += terms_ref[s].astype(F32)
    total += hidden_ref[...].astype(F32)
    residual_ref[...] = total
    inv = lax.rsqrt(jnp.mean(total * total, axis=1, keepdims=True) + EPSILON)
    normed_ref[...] = (total * inv * gain_ref[...]).astype(BF16)


def add_and_norm(table, terms, hidden, gain):
    outs = [(hidden.shape, F32), (hidden.shape, BF16)]
    return run(residual_kernel, table, [terms, hidden, gain], outs)


def gate_up_kernel(table_ref, near_ref, far_ref, *refs):
    *x_refs, out_ref, sums = refs
    side, _, _, depth = near_ref.shape
    sums[...] = jnp.zeros_like(sums)
    for at, w_ref in enumerate((near_ref, far_ref)):

        @pl.loop(0, side)
        def _(j, at=at, w_ref=w_ref):
            place = table_ref[WEIGHTS, at * side + j]
            cols = pl.ds(pl.multiple_of(place * depth, depth), depth)
            x = jnp.concatenate([ref[:, cols] for ref in x_refs], axis=0)
            sums[0] += dot(w_ref[j, 0], x, 1, 1)
            sums[1] += dot(w_ref[j, 1], x, 1, 1)

    gate = sums[0]
    out_ref[...] = (gate / (1.0 + jnp.exp(-gate)) * sums[1]).T.astype(BF16)


def gate_up(table, blocks, weights):
    count = rows_of(blocks)
    side, _, hidden, depth = weights[0].shape
    (out,) = run(
        gate_up_kernel,
        table,
        [*weights, *blocks],
        [((count, hidden), BF16)],
        8 * count * side * hidden * depth,
        scratch=[((2, hidden, count), F32)],
    )
    return out


def down_kernel(lanes, table_ref, x_ref, *refs):
    w_refs, out_refs = refs[:-lanes], refs[-lanes:]
    rows, side, width = x_ref.shape[0], w_refs[0].shape[0], w_refs[0].shape[2]
    for at, w_ref in enumerate(w_refs):

        @pl.loop(0, side)
        def _(j, at=at, w_ref=w_ref):
            acc = dot(x_ref[...], w_ref[j], 1, 0).reshape(rows // (8 * lanes), lanes, 8, width)
            place = table_ref[WEIGHTS, at * side + j]
            cols = pl.ds(pl.multiple_of(place * width, width), width)
            for s, ref in enumerate(out_refs):
                ref[:, cols] = acc[:, s].reshape(rows // lanes, width).astype(BF16)


def down(table, rows, weights, lanes):
    side, _, width = weights[0].shape
    shape = (rows.shape[0] // lanes, side * width * len(weights))
    return run(
        functools.partial(down_kernel, lanes), table, [rows, *weights], [(shape, BF16)] * lanes
    )


def sum_kernel(table_ref, *refs):
    *ins, out_ref = refs
    total = ins[0][...].astype(F32)
    for ref in ins[1:]:
        total += ref[...].astype(F32)
    groups, rows, width = out_ref.shape
    total = total.reshape(groups, rows, width)
    for s in range(groups):
        out_ref[table_ref[BLOCKS, s]] = total[s].astype(BF16)


def sum_pieces(table, pieces, groups):
    rows, width = pieces[0].shape
    outs = [((groups, rows // groups, width), BF16)]
    (out,) = run(sum_kernel, table, pieces, outs)
    return out


def per_device(
    hidden_in, gain_attn, w_qkv, cache_kv, cache_len, w_out, gain_mlp, w_gate_up, w_down
):
    depth, _, packed = w_qkv.shape
    seqs, spots = cache_kv.shape[:2]
    groups, lanes = lax.axis_size("z"), lax.axis_size("y")
    tied = lax.optimization_barrier
    w_qkv = w_qkv.reshape(depth, packed)
    gain_attn, gain_mlp = gain_attn.reshape(1, depth), gain_mlp.reshape(1, depth)
    cache = cache_kv.reshape(seqs, spots, cache_kv.shape[3])
    table = table_of_places(cache_len, seqs, spots)

    def gather_y(value):
        return tied(jnp.concatenate(gathered_turned(value, "y"), axis=0))

    def along_y(value):
        return [value] + [shifted(value, "y", -s) for s in range(1, lanes)]

    def exchanged(value, axis):
        return lax.all_to_all(value, axis, split_axis=0, concat_axis=0, tiled=True)

    r0 = gather_y(hidden_in)
    r0, w_gate_up, w_out, w_down = tied((r0, w_gate_up.transpose(1, 2, 0), w_out, w_down))
    f1, b1 = shifted(r0, "z", 1), shifted(r0, "z", -1)
    gates = gathered_turned(w_gate_up, "x")
    f2, b2 = shifted(f1, "z", 1), shifted(b1, "z", -1)
    w_heads = along_y(w_out)
    f3, b3 = shifted(f2, "z", 1), shifted(b2, "z", -1)
    f4 = shifted(f3, "z", 1)
    first = qkv_first(table, [r0, f1, b1, f2, b2], gain_attn, w_qkv)
    q, k, v = qkv_last(table, first, [f3, b3, f4], gain_attn, w_qkv)

    q = lax.all_gather(q, "c", axis=0, tiled=True)
    queries = gathered_turned(q, "x")
    parts = list(attend(table, (0,), queries[:1], k, v, cache))
    for slots in ((1, 3), (2,)):
        done = attend(table, slots, [queries[s] for s in slots], k, v, cache)
        parts += [shifted(part, "x", -s) for s, part in zip(slots, done)]
    mine, other = merge(table, parts)
    other = shifted(other, "c", 1)
    attended = combine(table, mine, other, lanes)

    attended, gates = tied((attended, gates))
    gates = jnp.stack(gates)
    gates = [gates, shifted(gates, "c", 1)]
    heads_here = exchanged(attended, "y")
    terms = project(table, heads_here, w_heads, groups)
    downs = gathered_turned(w_down, "x")
    terms = exchanged(terms, "z")
    residual, normed = add_and_norm(table, terms, hidden_in, gain_mlp)
    normed, gates = tied((normed, gates))

    r0 = gather_y(normed)
    f1, b1 = shifted(r0, "z", 1), shifted(r0, "z", -1)
    f2, b2 = shifted(f1, "z", 1), shifted(b1, "z", -1)
    f3, b3 = shifted(f2, "z", 1), shifted(b2, "z", -1)
    f3, downs = tied((f3, downs))
    downs = jnp.stack(downs)
    downs = [downs, shifted(downs, "c", 1)]
    f4 = shifted(f3, "z", 1)
    activated = gate_up(table, [r0, f1, b1, f2, b2, f3, b3, f4], gates)
    pieces = down(table, activated, downs, lanes)
    pieces = [shifted(piece, "y", -s) if s else piece for s, piece in enumerate(pieces)]
    shares = exchanged(sum_pieces(table, pieces, groups), "z")
    return (residual + shares.astype(F32).sum(axis=0)).astype(BF16)


def solution(mesh):
    split = Mesh(mesh.devices.reshape(8, 4, 4, 2), ("z", "y", "x", "c"))
    in_specs = (
        P(KV_TP, None),
        P(),
        P(None, TP, None),
        P(None, KV, TP, None),
        P(),
        P(TP, None),
        P(),
        P(KV, None, TP),
        P(TP, KV),
    )
    return jax.shard_map(
        per_device, mesh=split, in_specs=in_specs, out_specs=P(KV_TP, None), check_vma=False
    )
```

```python
import functools
import math

import jax
import jax.numpy as jnp
from jax import lax
from jax.experimental import pallas as pl
from jax.experimental.pallas import tpu as pltpu
from jax.sharding import Mesh
from jax.sharding import PartitionSpec as P


TP = ("z", "y")
KV = ("x", "c")
KV_TP = ("x", "c", "z", "y")

EPSILON = 1e-05
MASKED = -1e30
LOG2E = 1.4426950408889634
F32 = jnp.float32
BF16 = jnp.bfloat16


def shifted(value, axis, step):
    count = lax.axis_size(axis)
    return lax.ppermute(value, axis, [(i, (i + step) % count) for i in range(count)])


def gathered_turned(value, axis):
    return [value] + [shifted(value, axis, s) for s in range(1, lax.axis_size(axis))]


def dot(a, b, ca, cb):
    return lax.dot_general(a, b, (((ca,), (cb,)), ((), ())), preferred_element_type=F32)


def run(kernel, table, arrays, outs, flops=0, limit=16, scratch=()):
    return pl.pallas_call(
        kernel,
        in_specs=[pl.BlockSpec(memory_space=pltpu.SMEM)]
        + [pl.BlockSpec(memory_space=pltpu.VMEM)] * len(arrays),
        out_specs=[pl.BlockSpec(memory_space=pltpu.VMEM)] * len(outs),
        out_shape=[jax.ShapeDtypeStruct(shape, kind) for shape, kind in outs],
        scratch_shapes=[pltpu.VMEM(shape, kind) for shape, kind in scratch],
        compiler_params=pltpu.CompilerParams(vmem_limit_bytes=limit << 20),
        cost_estimate=pl.CostEstimate(flops=flops, transcendentals=0, bytes_accessed=0),
    )(table, *arrays)


WEIGHTS, BLOCKS, TURN, AHEAD, SEQ, LIMIT, OWN, CORE = range(8)


def table_of_places(cache_len, seqs, spots):
    groups, lanes, sides = lax.axis_size("z"), lax.axis_size("y"), lax.axis_size("x")
    x_at, c_at, z_at, y_at = (lax.axis_index(name) for name in ("x", "c", "z", "y"))
    step = jnp.arange(8, dtype=jnp.int32)
    x_from = (x_at + 2 * sides - step) & (sides - 1)
    seq = x_from // (sides // seqs)
    rows = [None] * 8
    rows[WEIGHTS] = 2 * x_from + ((c_at + step // sides) & 1)
    rows[BLOCKS] = (z_at + groups + (1 - 2 * (step & 1)) * ((step + 1) // 2)) & (groups - 1)
    rows[TURN] = (y_at + 2 * lanes - step) & (lanes - 1)
    rows[AHEAD] = (y_at + step) & (lanes - 1)
    rows[SEQ] = seq
    rows[LIMIT] = jnp.where(seq == 0, cache_len[0], cache_len[1]) - (2 * x_at + c_at) * spots
    rows[OWN] = (seq == x_at // (sides // seqs)).astype(jnp.int32)
    rows[CORE] = c_at + 0 * step
    return jnp.stack(rows)


def rows_of(blocks):
    return sum(block.shape[0] for block in blocks)


def project_rows(x_refs, gain_ref, w_ref):
    steps = 4
    width = w_ref.shape[0] // steps

    def chunk(j):
        cols = pl.ds(pl.multiple_of(j * width, width), width)
        return cols, jnp.concatenate([ref[:, cols] for ref in x_refs], axis=0).astype(F32)

    def squares(j, total):
        _, x = chunk(j)
        return total + jnp.sum(x * x, axis=1, keepdims=True)

    total = lax.fori_loop(0, steps, squares, jnp.zeros((rows_of(x_refs), 1), F32))
    inv = lax.rsqrt(total / w_ref.shape[0] + EPSILON)

    def body(j, acc):
        cols, x = chunk(j)
        return acc + dot((x * inv * gain_ref[:, cols]).astype(BF16), w_ref[cols], 1, 0)

    return lax.fori_loop(0, steps, body, jnp.zeros((rows_of(x_refs), w_ref.shape[1]), F32))


def qkv_first_kernel(table_ref, gain_ref, w_ref, *refs):
    *x_refs, out_ref = refs
    out_ref[...] = project_rows(x_refs, gain_ref, w_ref).astype(BF16)


def qkv_last_kernel(table_ref, gain_ref, w_ref, first_ref, *refs):
    *x_refs, q_ref, k_ref, v_ref = refs
    acc = project_rows(x_refs, gain_ref, w_ref).astype(BF16)
    size = q_ref.shape[1]
    done = first_ref.shape[0]
    for at, ref in enumerate((q_ref, k_ref, v_ref)):
        ref[:done] = first_ref[:, at * size : (at + 1) * size]
        ref[done:] = acc[:, at * size : (at + 1) * size]


def qkv_first(table, blocks, gain, weights):
    depth, packed = weights.shape
    count = rows_of(blocks)
    (out,) = run(
        qkv_first_kernel,
        table,
        [gain, weights, *blocks],
        [((count, packed), BF16)],
        2 * count * depth * packed,
    )
    return out


def qkv_last(table, first, blocks, gain, weights):
    depth, packed = weights.shape
    count = rows_of(blocks)
    return run(
        qkv_last_kernel,
        table,
        [gain, weights, first, *blocks],
        [((count + first.shape[0], packed // 3), BF16)] * 3,
        2 * count * depth * packed,
    )


def split3(value):
    first = value.astype(BF16).astype(F32)
    second = (value - first).astype(BF16).astype(F32)
    return first, second, value - first - second


def stats_of(peak, mass):
    row = lax.broadcasted_iota(jnp.int32, (16, peak.shape[1]), 0)
    stats = jnp.zeros((16, peak.shape[1]), F32)
    for at, part in enumerate(split3(peak) + split3(mass)):
        stats = jnp.where(row == at, part, stats)
    return stats.astype(BF16)


def attend_kernel(slots, table_ref, k_ref, v_ref, cache_ref, *refs):
    *refs, q_buf, out_buf = refs
    q_refs, out_refs = refs[: len(slots)], refs[len(slots) :]
    blocks, size = k_ref.shape
    scale = LOG2E / math.sqrt(size)
    halves = q_buf.shape[1] // blocks
    for at, ref in enumerate(q_refs):
        q_buf[at] = ref[...]

    @pl.loop(0, len(slots) * halves)
    def _(turn):
        which, half = turn // halves, turn % halves
        slot = slots[0] + which * (slots[-1] - slots[0])
        seq = table_ref[SEQ, slot]
        limit = table_ref[LIMIT, slot]
        own = table_ref[OWN, slot] > 0
        at = pl.ds(pl.multiple_of(half * blocks, blocks), blocks)
        q = q_buf[which, at]
        s1 = dot(cache_ref[seq, :, :size], q, 1, 1) * scale
        s2 = dot(k_ref[...], q, 1, 1) * scale
        usable = lax.broadcasted_iota(jnp.int32, s1.shape, 0) < limit
        s1 = jnp.where(usable, s1, MASKED)
        s2 = jnp.where(own, s2, MASKED)
        top = jnp.maximum(jnp.max(s1, axis=0, keepdims=True), jnp.max(s2, axis=0, keepdims=True))
        peak = jnp.maximum(top, 0.1 * MASKED)
        p1 = jnp.exp2(s1 - peak)
        p2 = jnp.exp2(s2 - peak)
        mass = jnp.sum(p1, axis=0, keepdims=True) + jnp.sum(p2, axis=0, keepdims=True)
        acc = dot(cache_ref[seq, :, size:], p1.astype(BF16), 0, 0)
        acc += dot(v_ref[...], p2.astype(BF16), 0, 0)
        out_buf[which, :size, at] = acc.astype(BF16)
        out_buf[which, size:, at] = stats_of(peak, mass)

    for at, ref in enumerate(out_refs):
        ref[...] = out_buf[at]


def attend(table, slots, queries, k, v, cache):
    count, size = k.shape
    rows = queries[0].shape[0]
    return run(
        functools.partial(attend_kernel, slots),
        table,
        [k, v, cache, *queries],
        [((size + 16, rows), BF16)] * len(slots),
        4 * rows_of(queries) * size * (cache.shape[1] + count),
        scratch=[((len(slots), rows, size), BF16), ((len(slots), size + 16, rows), BF16)],
    )


def merged(parts, size):
    stats = [part[size:].astype(F32) for part in parts]
    peaks = [s[0:1] + s[1:2] + s[2:3] for s in stats]
    best = functools.reduce(jnp.maximum, peaks)
    mass = jnp.zeros_like(best)
    acc = jnp.zeros((size, best.shape[1]), F32)
    for part, s, peak in zip(parts, stats, peaks):
        scaling = jnp.exp2(peak - best)
        mass += (s[3:4] + s[4:5] + s[5:6]) * scaling
        acc += part[:size].astype(F32) * scaling
    return best, mass, acc


def merge_kernel(table_ref, *refs):
    *parts, mine_ref, other_ref = refs
    height, width = mine_ref.shape
    size = height - 16
    core = table_ref[CORE, 0]
    for ref, side in ((mine_ref, core), (other_ref, 1 - core)):
        cols = pl.ds(pl.multiple_of(side * width, width), width)
        best, mass, acc = merged([part[:, cols] for part in parts], size)
        ref[:size] = acc.astype(BF16)
        ref[size:] = stats_of(best, mass)


def merge(table, parts):
    height, width = parts[0].shape
    return run(merge_kernel, table, parts, [((height, width // 2), BF16)] * 2)


def combine_kernel(table_ref, mine_ref, other_ref, out_ref):
    size = mine_ref.shape[0] - 16
    lanes, rows, _ = out_ref.shape
    _, mass, acc = merged([mine_ref[...], other_ref[...]], size)
    attended = (acc / mass).T.reshape(rows // 8, lanes, 8, size)
    for s in range(lanes):
        out_ref[table_ref[TURN, s]] = attended[:, s].reshape(rows, size).astype(BF16)


def combine(table, mine, other, lanes):
    height, width = mine.shape
    shape = (lanes, width // lanes, height - 16)
    (out,) = run(combine_kernel, table, [mine, other], [(shape, BF16)])
    return out


def project_kernel(table_ref, heads_ref, *refs):
    *w_refs, out_ref = refs
    groups, rows, width = out_ref.shape
    heads = jnp.concatenate(
        [heads_ref[table_ref[AHEAD, s]] for s in range(len(w_refs))], axis=1
    )
    tile = width // 4

    @pl.loop(0, 4)
    def _(j):
        cols = pl.ds(pl.multiple_of(j * tile, tile), tile)
        acc = dot(heads, jnp.concatenate([w[:, cols] for w in w_refs], axis=0), 1, 0)
        acc = acc.reshape(groups, rows, tile)
        for s in range(groups):
            out_ref[table_ref[BLOCKS, s], :, cols] = acc[s].astype(BF16)


def project(table, heads, weights, groups):
    _, rows, _ = heads.shape
    shape = (groups, rows // groups, weights[0].shape[1])
    (out,) = run(project_kernel, table, [heads, *weights], [(shape, BF16)])
    return out


def residual_kernel(table_ref, terms_ref, hidden_ref, gain_ref, residual_ref, normed_ref):
    total = terms_ref[0].astype(F32)
    for s in range(1, terms_ref.shape[0]):
        total += terms_ref[s].astype(F32)
    total += hidden_ref[...].astype(F32)
    residual_ref[...] = total
    inv = lax.rsqrt(jnp.mean(total * total, axis=1, keepdims=True) + EPSILON)
    normed_ref[...] = (total * inv * gain_ref[...]).astype(BF16)


def add_and_norm(table, terms, hidden, gain):
    outs = [(hidden.shape, F32), (hidden.shape, BF16)]
    return run(residual_kernel, table, [terms, hidden, gain], outs)


def gate_up_kernel(table_ref, near_ref, far_ref, *refs):
    *x_refs, out_ref, sums = refs
    side, _, _, depth = near_ref.shape
    sums[...] = jnp.zeros_like(sums)
    for at, w_ref in enumerate((near_ref, far_ref)):

        @pl.loop(0, side)
        def _(j, at=at, w_ref=w_ref):
            place = table_ref[WEIGHTS, at * side + j]
            cols = pl.ds(pl.multiple_of(place * depth, depth), depth)
            x = jnp.concatenate([ref[:, cols] for ref in x_refs], axis=0)
            sums[0] += dot(w_ref[j, 0], x, 1, 1)
            sums[1] += dot(w_ref[j, 1], x, 1, 1)

    gate = sums[0]
    out_ref[...] = (gate / (1.0 + jnp.exp(-gate)) * sums[1]).T.astype(BF16)


def gate_up(table, blocks, weights):
    count = rows_of(blocks)
    side, _, hidden, depth = weights[0].shape
    (out,) = run(
        gate_up_kernel,
        table,
        [*weights, *blocks],
        [((count, hidden), BF16)],
        8 * count * side * hidden * depth,
        scratch=[((2, hidden, count), F32)],
    )
    return out


def down_kernel(lanes, table_ref, x_ref, *refs):
    w_refs, out_refs = refs[:-lanes], refs[-lanes:]
    rows, side, width = x_ref.shape[0], w_refs[0].shape[0], w_refs[0].shape[2]
    for at, w_ref in enumerate(w_refs):

        @pl.loop(0, side)
        def _(j, at=at, w_ref=w_ref):
            acc = dot(x_ref[...], w_ref[j], 1, 0).reshape(rows // (8 * lanes), lanes, 8, width)
            place = table_ref[WEIGHTS, at * side + j]
            cols = pl.ds(pl.multiple_of(place * width, width), width)
            for s, ref in enumerate(out_refs):
                ref[:, cols] = acc[:, s].reshape(rows // lanes, width).astype(BF16)


def down(table, rows, weights, lanes):
    side, _, width = weights[0].shape
    shape = (rows.shape[0] // lanes, side * width * len(weights))
    return run(
        functools.partial(down_kernel, lanes),
        table,
        [rows, *weights],
        [(shape, BF16)] * lanes,
    )


def sum_kernel(table_ref, *refs):
    *ins, out_ref = refs
    total = ins[0][...].astype(F32)
    for ref in ins[1:]:
        total += ref[...].astype(F32)
    groups, rows, width = out_ref.shape
    total = total.reshape(groups, rows, width)
    for s in range(groups):
        out_ref[table_ref[BLOCKS, s]] = total[s].astype(BF16)


def sum_pieces(table, pieces, groups):
    rows, width = pieces[0].shape
    outs = [((groups, rows // groups, width), BF16)]
    (out,) = run(sum_kernel, table, pieces, outs)
    return out


def per_device(
    hidden_in, gain_attn, w_qkv, cache_kv, cache_len, w_out, gain_mlp, w_gate_up, w_down
):
    depth, _, packed = w_qkv.shape
    seqs, spots = cache_kv.shape[:2]
    groups, lanes = lax.axis_size("z"), lax.axis_size("y")
    tied = lax.optimization_barrier
    w_qkv = w_qkv.reshape(depth, packed)
    gain_attn, gain_mlp = gain_attn.reshape(1, depth), gain_mlp.reshape(1, depth)
    cache = cache_kv.reshape(seqs, spots, cache_kv.shape[3])
    table = table_of_places(cache_len, seqs, spots)

    def gather_y(value):
        return tied(jnp.concatenate(gathered_turned(value, "y"), axis=0))

    def along_y(value):
        return [value] + [shifted(value, "y", -s) for s in range(1, lanes)]

    def exchanged(value, axis):
        return lax.all_to_all(value, axis, split_axis=0, concat_axis=0, tiled=True)

    r0 = gather_y(hidden_in)
    r0, w_out, w_down = tied((r0, w_out, w_down))
    f1, b1 = shifted(r0, "z", 1), shifted(r0, "z", -1)
    gates = gathered_turned(w_gate_up.transpose(1, 2, 0), "x")
    f2, b2 = shifted(f1, "z", 1), shifted(b1, "z", -1)
    w_heads = along_y(w_out)
    f3, b3 = shifted(f2, "z", 1), shifted(b2, "z", -1)
    f4 = shifted(f3, "z", 1)
    first = qkv_first(table, [r0, f1, b1, f2, b2], gain_attn, w_qkv)
    q, k, v = qkv_last(table, first, [f3, b3, f4], gain_attn, w_qkv)

    q = lax.all_gather(q, "c", axis=0, tiled=True)
    queries = gathered_turned(q, "x")
    parts = list(attend(table, (0,), queries[:1], k, v, cache))
    for slots in ((1, 3), (2,)):
        done = attend(table, slots, [queries[s] for s in slots], k, v, cache)
        parts += [shifted(part, "x", -s) for s, part in zip(slots, done)]
    mine, other = merge(table, parts)
    other = shifted(other, "c", 1)
    attended = combine(table, mine, other, lanes)

    attended, gates = tied((attended, gates))
    gates = jnp.stack(gates)
    gates = [gates, shifted(gates, "c", 1)]
    heads_here = exchanged(attended, "y")
    terms = project(table, heads_here, w_heads, groups)
    downs = gathered_turned(w_down, "x")
    terms = exchanged(terms, "z")
    residual, normed = add_and_norm(table, terms, hidden_in, gain_mlp)
    normed, gates = tied((normed, gates))

    r0 = gather_y(normed)
    f1, b1 = shifted(r0, "z", 1), shifted(r0, "z", -1)
    f2, b2 = shifted(f1, "z", 1), shifted(b1, "z", -1)
    f3, b3 = shifted(f2, "z", 1), shifted(b2, "z", -1)
    downs = jnp.stack(downs)
    downs = [downs, shifted(downs, "c", 1)]
    f4 = shifted(f3, "z", 1)
    activated = gate_up(table, [r0, f1, b1, f2, b2, f3, b3, f4], gates)
    pieces = down(table, activated, downs, lanes)
    pieces = [shifted(piece, "y", -s) if s else piece for s, piece in enumerate(pieces)]
    shares = exchanged(sum_pieces(table, pieces, groups), "z")
    return (residual + shares.astype(F32).sum(axis=0)).astype(BF16)


def solution(mesh):
    split = Mesh(mesh.devices.reshape(8, 4, 4, 2), ("z", "y", "x", "c"))
    in_specs = (
        P(KV_TP, None),
        P(),
        P(None, TP, None),
        P(None, KV, TP, None),
        P(),
        P(TP, None),
        P(),
        P(KV, None, TP),
        P(TP, KV),
    )
    return jax.shard_map(
        per_device, mesh=split, in_specs=in_specs, out_specs=P(KV_TP, None), check_vma=False
    )
```

```python
import functools
import math

import jax
import jax.numpy as jnp
from jax import lax
from jax.experimental import pallas as pl
from jax.experimental.pallas import tpu as pltpu
from jax.sharding import Mesh
from jax.sharding import PartitionSpec as P


TP = ("z", "y")
KV = ("x", "c")
KV_TP = ("x", "c", "z", "y")

EPSILON = 1e-05
MASKED = -1e30
LOG2E = 1.4426950408889634
F32 = jnp.float32
BF16 = jnp.bfloat16


def shifted(value, axis, step):
    count = lax.axis_size(axis)
    return lax.ppermute(value, axis, [(i, (i + step) % count) for i in range(count)])


def gathered_turned(value, axis):
    return [value] + [shifted(value, axis, s) for s in range(1, lax.axis_size(axis))]


def dot(a, b, ca, cb):
    return lax.dot_general(a, b, (((ca,), (cb,)), ((), ())), preferred_element_type=F32)


def run(kernel, table, arrays, outs, flops=0, limit=16, scratch=(), far=0, sems=0):
    return pl.pallas_call(
        kernel,
        in_specs=[pl.BlockSpec(memory_space=pltpu.SMEM)]
        + [pl.BlockSpec(memory_space=pltpu.HBM)] * far
        + [pl.BlockSpec(memory_space=pltpu.VMEM)] * (len(arrays) - far),
        out_specs=[pl.BlockSpec(memory_space=pltpu.VMEM)] * len(outs),
        out_shape=[jax.ShapeDtypeStruct(shape, kind) for shape, kind in outs],
        scratch_shapes=[pltpu.VMEM(shape, kind) for shape, kind in scratch]
        + ([pltpu.SemaphoreType.DMA((sems,))] if sems else []),
        compiler_params=pltpu.CompilerParams(vmem_limit_bytes=limit << 20),
        cost_estimate=pl.CostEstimate(flops=flops, transcendentals=0, bytes_accessed=0),
    )(table, *arrays)


WEIGHTS, BLOCKS, TURN, AHEAD, SEQ, LIMIT, OWN, CORE = range(8)


def table_of_places(cache_len, seqs, spots):
    groups, lanes, sides = lax.axis_size("z"), lax.axis_size("y"), lax.axis_size("x")
    x_at, c_at, z_at, y_at = (lax.axis_index(name) for name in ("x", "c", "z", "y"))
    step = jnp.arange(8, dtype=jnp.int32)
    x_from = (x_at + 2 * sides - step) & (sides - 1)
    seq = x_from // (sides // seqs)
    rows = [None] * 8
    rows[WEIGHTS] = 2 * x_from + ((c_at + step // sides) & 1)
    rows[BLOCKS] = (z_at + groups + (1 - 2 * (step & 1)) * ((step + 1) // 2)) & (groups - 1)
    rows[TURN] = (y_at + 2 * lanes - step) & (lanes - 1)
    rows[AHEAD] = (y_at + step) & (lanes - 1)
    rows[SEQ] = seq
    rows[LIMIT] = jnp.where(seq == 0, cache_len[0], cache_len[1]) - (2 * x_at + c_at) * spots
    rows[OWN] = (seq == x_at // (sides // seqs)).astype(jnp.int32)
    rows[CORE] = c_at + 0 * step
    return jnp.stack(rows)


def rows_of(blocks):
    return sum(block.shape[0] for block in blocks)


def project_rows(x_refs, gain_ref, w_ref):
    steps = 4
    width = w_ref.shape[0] // steps

    def chunk(j):
        cols = pl.ds(pl.multiple_of(j * width, width), width)
        return cols, jnp.concatenate([ref[:, cols] for ref in x_refs], axis=0).astype(F32)

    def squares(j, total):
        _, x = chunk(j)
        return total + jnp.sum(x * x, axis=1, keepdims=True)

    total = lax.fori_loop(0, steps, squares, jnp.zeros((rows_of(x_refs), 1), F32))
    inv = lax.rsqrt(total / w_ref.shape[0] + EPSILON)

    def body(j, acc):
        cols, x = chunk(j)
        return acc + dot((x * inv * gain_ref[:, cols]).astype(BF16), w_ref[cols], 1, 0)

    return lax.fori_loop(0, steps, body, jnp.zeros((rows_of(x_refs), w_ref.shape[1]), F32))


def qkv_first_kernel(table_ref, gain_ref, w_ref, *refs):
    *x_refs, out_ref = refs
    out_ref[...] = project_rows(x_refs, gain_ref, w_ref).astype(BF16)


def qkv_last_kernel(table_ref, gain_ref, w_ref, first_ref, *refs):
    *x_refs, q_ref, k_ref, v_ref = refs
    acc = project_rows(x_refs, gain_ref, w_ref).astype(BF16)
    size = q_ref.shape[1]
    done = first_ref.shape[0]
    for at, ref in enumerate((q_ref, k_ref, v_ref)):
        ref[:done] = first_ref[:, at * size : (at + 1) * size]
        ref[done:] = acc[:, at * size : (at + 1) * size]


def qkv_first(table, blocks, gain, weights):
    depth, packed = weights.shape
    count = rows_of(blocks)
    (out,) = run(
        qkv_first_kernel,
        table,
        [gain, weights, *blocks],
        [((count, packed), BF16)],
        2 * count * depth * packed,
    )
    return out


def qkv_last(table, first, blocks, gain, weights):
    depth, packed = weights.shape
    count = rows_of(blocks)
    return run(
        qkv_last_kernel,
        table,
        [gain, weights, first, *blocks],
        [((count + first.shape[0], packed // 3), BF16)] * 3,
        2 * count * depth * packed,
    )


def split3(value):
    first = value.astype(BF16).astype(F32)
    second = (value - first).astype(BF16).astype(F32)
    return first, second, value - first - second


def stats_of(peak, mass):
    row = lax.broadcasted_iota(jnp.int32, (16, peak.shape[1]), 0)
    stats = jnp.zeros((16, peak.shape[1]), F32)
    for at, part in enumerate(split3(peak) + split3(mass)):
        stats = jnp.where(row == at, part, stats)
    return stats.astype(BF16)


def attend_kernel(slots, table_ref, k_ref, v_ref, cache_ref, *refs):
    *refs, q_buf, out_buf = refs
    q_refs, out_refs = refs[: len(slots)], refs[len(slots) :]
    blocks, size = k_ref.shape
    scale = LOG2E / math.sqrt(size)
    halves = q_buf.shape[1] // blocks
    for at, ref in enumerate(q_refs):
        q_buf[at] = ref[...]

    @pl.loop(0, len(slots) * halves)
    def _(turn):
        which, half = turn // halves, turn % halves
        slot = slots[0] + which * (slots[-1] - slots[0])
        seq = table_ref[SEQ, slot]
        limit = table_ref[LIMIT, slot]
        own = table_ref[OWN, slot] > 0
        at = pl.ds(pl.multiple_of(half * blocks, blocks), blocks)
        q = q_buf[which, at]
        s1 = dot(cache_ref[seq, :, :size], q, 1, 1) * scale
        s2 = dot(k_ref[...], q, 1, 1) * scale
        usable = lax.broadcasted_iota(jnp.int32, s1.shape, 0) < limit
        s1 = jnp.where(usable, s1, MASKED)
        s2 = jnp.where(own, s2, MASKED)
        top = jnp.maximum(jnp.max(s1, axis=0, keepdims=True), jnp.max(s2, axis=0, keepdims=True))
        peak = jnp.maximum(top, 0.1 * MASKED)
        p1 = jnp.exp2(s1 - peak)
        p2 = jnp.exp2(s2 - peak)
        mass = jnp.sum(p1, axis=0, keepdims=True) + jnp.sum(p2, axis=0, keepdims=True)
        acc = dot(cache_ref[seq, :, size:], p1.astype(BF16), 0, 0)
        acc += dot(v_ref[...], p2.astype(BF16), 0, 0)
        out_buf[which, :size, at] = acc.astype(BF16)
        out_buf[which, size:, at] = stats_of(peak, mass)

    for at, ref in enumerate(out_refs):
        ref[...] = out_buf[at]


def attend(table, slots, queries, k, v, cache):
    count, size = k.shape
    rows = queries[0].shape[0]
    return run(
        functools.partial(attend_kernel, slots),
        table,
        [k, v, cache, *queries],
        [((size + 16, rows), BF16)] * len(slots),
        4 * rows_of(queries) * size * (cache.shape[1] + count),
        scratch=[((len(slots), rows, size), BF16), ((len(slots), size + 16, rows), BF16)],
    )


def merged(parts, size):
    stats = [part[size:].astype(F32) for part in parts]
    peaks = [s[0:1] + s[1:2] + s[2:3] for s in stats]
    best = functools.reduce(jnp.maximum, peaks)
    mass = jnp.zeros_like(best)
    acc = jnp.zeros((size, best.shape[1]), F32)
    for part, s, peak in zip(parts, stats, peaks):
        scaling = jnp.exp2(peak - best)
        mass += (s[3:4] + s[4:5] + s[5:6]) * scaling
        acc += part[:size].astype(F32) * scaling
    return best, mass, acc


def merge_kernel(table_ref, *refs):
    *parts, mine_ref, other_ref = refs
    height, width = mine_ref.shape
    size = height - 16
    core = table_ref[CORE, 0]
    for ref, side in ((mine_ref, core), (other_ref, 1 - core)):
        cols = pl.ds(pl.multiple_of(side * width, width), width)
        best, mass, acc = merged([part[:, cols] for part in parts], size)
        ref[:size] = acc.astype(BF16)
        ref[size:] = stats_of(best, mass)


def merge(table, parts):
    height, width = parts[0].shape
    return run(merge_kernel, table, parts, [((height, width // 2), BF16)] * 2)


def combine_kernel(table_ref, mine_ref, other_ref, out_ref):
    size = mine_ref.shape[0] - 16
    lanes, rows, _ = out_ref.shape
    _, mass, acc = merged([mine_ref[...], other_ref[...]], size)
    attended = (acc / mass).T.reshape(rows // 8, lanes, 8, size)
    for s in range(lanes):
        out_ref[table_ref[TURN, s]] = attended[:, s].reshape(rows, size).astype(BF16)


def combine(table, mine, other, lanes):
    height, width = mine.shape
    shape = (lanes, width // lanes, height - 16)
    (out,) = run(combine_kernel, table, [mine, other], [(shape, BF16)])
    return out


def project_kernel(table_ref, heads_ref, *refs):
    *w_refs, out_ref = refs
    groups, rows, width = out_ref.shape
    heads = jnp.concatenate(
        [heads_ref[table_ref[AHEAD, s]] for s in range(len(w_refs))], axis=1
    )
    tile = width // 4

    @pl.loop(0, 4)
    def _(j):
        cols = pl.ds(pl.multiple_of(j * tile, tile), tile)
        acc = dot(heads, jnp.concatenate([w[:, cols] for w in w_refs], axis=0), 1, 0)
        acc = acc.reshape(groups, rows, tile)
        for s in range(groups):
            out_ref[table_ref[BLOCKS, s], :, cols] = acc[s].astype(BF16)


def project(table, heads, weights, groups):
    _, rows, _ = heads.shape
    shape = (groups, rows // groups, weights[0].shape[1])
    (out,) = run(project_kernel, table, [heads, *weights], [(shape, BF16)])
    return out


def residual_kernel(table_ref, terms_ref, hidden_ref, gain_ref, residual_ref, normed_ref):
    total = terms_ref[0].astype(F32)
    for s in range(1, terms_ref.shape[0]):
        total += terms_ref[s].astype(F32)
    total += hidden_ref[...].astype(F32)
    residual_ref[...] = total
    inv = lax.rsqrt(jnp.mean(total * total, axis=1, keepdims=True) + EPSILON)
    normed_ref[...] = (total * inv * gain_ref[...]).astype(BF16)


def add_and_norm(table, terms, hidden, gain):
    outs = [(hidden.shape, F32), (hidden.shape, BF16)]
    return run(residual_kernel, table, [terms, hidden, gain], outs)


def gate_up_kernel(table_ref, near_ref, far_ref, *refs):
    *x_refs, out_ref, sums, w_buf, sems = refs
    side, _, _, depth = near_ref.shape
    for at, ref in enumerate((near_ref, far_ref)):
        for j in range(side):
            place = at * side + j
            pltpu.make_async_copy(ref.at[j], w_buf.at[place], sems.at[place]).start()
    sums[...] = jnp.zeros_like(sums)

    @pl.loop(0, 2 * side)
    def _(j):
        cols = pl.ds(pl.multiple_of(table_ref[WEIGHTS, j] * depth, depth), depth)
        x = jnp.concatenate([ref[:, cols] for ref in x_refs], axis=0)
        pltpu.make_async_copy(w_buf.at[j], w_buf.at[j], sems.at[j]).wait()
        sums[0] += dot(w_buf[j, 0], x, 1, 1)
        sums[1] += dot(w_buf[j, 1], x, 1, 1)

    gate = sums[0]
    out_ref[...] = (gate / (1.0 + jnp.exp(-gate)) * sums[1]).T.astype(BF16)


def gate_up(table, blocks, weights):
    count = rows_of(blocks)
    side, _, hidden, depth = weights[0].shape
    (out,) = run(
        gate_up_kernel,
        table,
        [*weights, *blocks],
        [((count, hidden), BF16)],
        8 * count * side * hidden * depth,
        scratch=[((2, hidden, count), F32), ((2 * side, 2, hidden, depth), BF16)],
        far=2,
        sems=2 * side,
    )
    return out


def down_kernel(lanes, table_ref, x_ref, *refs):
    w_refs, out_refs = refs[:-lanes], refs[-lanes:]
    rows, side, width = x_ref.shape[0], w_refs[0].shape[0], w_refs[0].shape[2]
    for at, w_ref in enumerate(w_refs):

        @pl.loop(0, side)
        def _(j, at=at, w_ref=w_ref):
            acc = dot(x_ref[...], w_ref[j], 1, 0).reshape(rows // (8 * lanes), lanes, 8, width)
            place = table_ref[WEIGHTS, at * side + j]
            cols = pl.ds(pl.multiple_of(place * width, width), width)
            for s, ref in enumerate(out_refs):
                ref[:, cols] = acc[:, s].reshape(rows // lanes, width).astype(BF16)


def down(table, rows, weights, lanes):
    side, _, width = weights[0].shape
    shape = (rows.shape[0] // lanes, side * width * len(weights))
    return run(
        functools.partial(down_kernel, lanes), table, [rows, *weights], [(shape, BF16)] * lanes
    )


def sum_kernel(table_ref, *refs):
    *ins, out_ref = refs
    total = ins[0][...].astype(F32)
    for ref in ins[1:]:
        total += ref[...].astype(F32)
    groups, rows, width = out_ref.shape
    total = total.reshape(groups, rows, width)
    for s in range(groups):
        out_ref[table_ref[BLOCKS, s]] = total[s].astype(BF16)


def sum_pieces(table, pieces, groups):
    rows, width = pieces[0].shape
    outs = [((groups, rows // groups, width), BF16)]
    (out,) = run(sum_kernel, table, pieces, outs)
    return out


def per_device(
    hidden_in, gain_attn, w_qkv, cache_kv, cache_len, w_out, gain_mlp, w_gate_up, w_down
):
    depth, _, packed = w_qkv.shape
    seqs, spots = cache_kv.shape[:2]
    groups, lanes = lax.axis_size("z"), lax.axis_size("y")
    tied = lax.optimization_barrier
    w_qkv = w_qkv.reshape(depth, packed)
    gain_attn, gain_mlp = gain_attn.reshape(1, depth), gain_mlp.reshape(1, depth)
    cache = cache_kv.reshape(seqs, spots, cache_kv.shape[3])
    table = table_of_places(cache_len, seqs, spots)

    def gather_y(value):
        return tied(jnp.concatenate(gathered_turned(value, "y"), axis=0))

    def along_y(value):
        return [value] + [shifted(value, "y", -s) for s in range(1, lanes)]

    def exchanged(value, axis):
        return lax.all_to_all(value, axis, split_axis=0, concat_axis=0, tiled=True)

    r0 = gather_y(hidden_in)
    r0, w_out, w_down = tied((r0, w_out, w_down))
    f1, b1 = shifted(r0, "z", 1), shifted(r0, "z", -1)
    gates = gathered_turned(w_gate_up.transpose(1, 2, 0), "x")
    f2, b2 = shifted(f1, "z", 1), shifted(b1, "z", -1)
    w_heads = along_y(w_out)
    f3, b3 = shifted(f2, "z", 1), shifted(b2, "z", -1)
    f4 = shifted(f3, "z", 1)
    first = qkv_first(table, [r0, f1, b1, f2, b2], gain_attn, w_qkv)
    q, k, v = qkv_last(table, first, [f3, b3, f4], gain_attn, w_qkv)

    q = lax.all_gather(q, "c", axis=0, tiled=True)
    q_far = shifted(q, "x", 2)
    queries = [q, shifted(q, "x", 1), q_far, shifted(q, "x", 3)]
    parts = list(attend(table, (0,), queries[:1], k, v, cache))
    for slots in ((2,), (1, 3)):
        done = attend(table, slots, [queries[s] for s in slots], k, v, cache)
        parts += [shifted(part, "x", -s) for s, part in zip(slots, done)]
    mine, other = merge(table, parts)
    other = shifted(other, "c", 1)
    attended = combine(table, mine, other, lanes)

    gates = jnp.stack(gates)
    gates = [gates, shifted(gates, "c", 1)]
    heads_here = exchanged(attended, "y")
    terms = project(table, heads_here, w_heads, groups)
    downs = gathered_turned(w_down, "x")
    terms = exchanged(terms, "z")
    residual, normed = add_and_norm(table, terms, hidden_in, gain_mlp)
    normed, gates = tied((normed, gates))

    r0 = gather_y(normed)
    f1, b1 = shifted(r0, "z", 1), shifted(r0, "z", -1)
    f2, b2 = shifted(f1, "z", 1), shifted(b1, "z", -1)
    f3, b3 = shifted(f2, "z", 1), shifted(b2, "z", -1)
    downs = jnp.stack(downs)
    downs = [downs, shifted(downs, "c", 1)]
    f4 = shifted(f3, "z", 1)
    activated = gate_up(table, [r0, f1, b1, f2, b2, f3, b3, f4], gates)
    pieces = down(table, activated, downs, lanes)
    pieces = [shifted(piece, "y", -s) if s else piece for s, piece in enumerate(pieces)]
    shares = exchanged(sum_pieces(table, pieces, groups), "z")
    return (residual + shares.astype(F32).sum(axis=0)).astype(BF16)


def solution(mesh):
    split = Mesh(mesh.devices.reshape(8, 4, 4, 2), ("z", "y", "x", "c"))
    in_specs = (
        P(KV_TP, None),
        P(),
        P(None, TP, None),
        P(None, KV, TP, None),
        P(),
        P(TP, None),
        P(),
        P(KV, None, TP),
        P(TP, KV),
    )
    return jax.shard_map(
        per_device, mesh=split, in_specs=in_specs, out_specs=P(KV_TP, None), check_vma=False
    )
```
